32 devices in a mesh: dp: 4 (over x, y), tp: 8 (over z, core).
Axes of the slice: x: 2, y: 2, z: 4, core: 2. Of those that a mesh axis runs over, the one named last changes fastest.
Arguments:
- hidden: bfloat16 [256, 4, 1536], P('dp'), parts along dimension 0
- norm_gain: float32 [1536], replicated
- w_head: bfloat16 [1536, 151936], P(None, 'tp')
- draft_probs: float32 [256, 3, 151936], P('dp', None, 'tp'), parts along dimension 0
- draft_tokens: int32 [256, 3], P('dp'), parts along dimension 0
- temperature: float32 [256], P('dp'), parts along dimension 0
Outputs:
- output 1: float32 [256, 3], P('dp'), parts along dimension 0
- output 2: float32 [256, 3], P('dp'), parts along dimension 0
- output 3: float32 [256, 3, 151936], P('dp', None, 'tp'), parts along dimension 0
- output 4: float32 [256], P('dp'), parts along dimension 0
There are 4 independent parts. The reference program is written for one: setup_inputs(seed, part) draws one part's arguments, and reference() takes and returns one part's arrays. A program takes and returns all parts, laid end to end along the dimension named above; an argument that names none is the same for every part.
All inputs are finite; a program needn't handle non-finite values.
Results may differ from the reference program's by a relative error of at most 0.001.
Values sent between devices are 32-bit elements.
A program may use at most 1 GiB of HBM per device.

```python
import jax
import jax.numpy as jnp
from jax import lax

BATCH_ROWS = 64
DRAFT_LEN = 3
D_MODEL = 1536
VOCAB_SIZE = 151936
CLUSTER_COUNT = 3
WEIGHT_BLOCK = 128
CLUSTER_SPAN = VOCAB_SIZE // 32


def setup_inputs(seed: int = 0, part: int = 0) -> dict:
    part_key = jax.random.fold_in(jax.random.key(seed), part)
    key_h, key_q, key_s, key_t, key_c, key_k, key_o = jax.random.split(part_key, 7)
    key_w, key_g = jax.random.split(jax.random.key(seed + 1), 2)
    hidden = jax.random.normal(key_h, (BATCH_ROWS, DRAFT_LEN + 1, D_MODEL), jnp.float32).astype(jnp.bfloat16)
    norm_gain = jax.random.uniform(key_g, (D_MODEL,), jnp.float32, 0.5, 1.5)

    def weight_block(block_idx):
        gauss_block = jax.random.normal(jax.random.fold_in(key_w, block_idx), (WEIGHT_BLOCK, VOCAB_SIZE), jnp.float32)
        return (gauss_block * D_MODEL ** -0.5).astype(jnp.bfloat16)

    w_head = lax.map(weight_block, jnp.arange(D_MODEL // WEIGHT_BLOCK)).reshape(D_MODEL, VOCAB_SIZE)
    q_scale = jax.random.uniform(key_s, (BATCH_ROWS, DRAFT_LEN, 1), jnp.float32, 0.7, 1.3)
    q_logits = jax.random.normal(key_q, (BATCH_ROWS, DRAFT_LEN, VOCAB_SIZE), jnp.float32) * q_scale
    draft_probs = jax.nn.softmax(q_logits, axis=-1)
    temperature = jax.random.uniform(key_t, (BATCH_ROWS,), jnp.float32, 0.6, 1.4)
    centers = jax.random.randint(key_c, (CLUSTER_COUNT,), 0, VOCAB_SIZE - CLUSTER_SPAN)
    choice = jax.random.randint(key_k, (BATCH_ROWS, DRAFT_LEN), 0, CLUSTER_COUNT)
    offsets = jax.random.randint(key_o, (BATCH_ROWS, DRAFT_LEN), 0, CLUSTER_SPAN)
    draft_tokens = (centers[choice] + offsets).astype(jnp.int32)
    return {'hidden': hidden, 'norm_gain': norm_gain, 'w_head': w_head, 'draft_probs': draft_probs, 'draft_tokens': draft_tokens, 'temperature': temperature}


def reference(hidden, norm_gain, w_head, draft_probs, draft_tokens, temperature):
    def one_row(row_args):
        row_hidden, row_probs, row_tokens, row_temp = row_args
        hidden_f32 = row_hidden.astype(jnp.float32)
        inv_rms = lax.rsqrt(jnp.mean(hidden_f32 * hidden_f32, axis=-1, keepdims=True) + 1e-5)
        normed = (hidden_f32 * inv_rms * norm_gain).astype(jnp.bfloat16)
        logits = jnp.dot(normed, w_head, preferred_element_type=jnp.float32)
        scaled = logits / row_temp
        row_max = jnp.max(scaled, axis=-1, keepdims=True)
        row_lse = row_max + jnp.log(jnp.sum(jnp.exp(scaled - row_max), axis=-1, keepdims=True))
        target = jnp.exp(scaled[:DRAFT_LEN] - row_lse[:DRAFT_LEN])
        tok_target = jnp.take_along_axis(target, row_tokens[:, None], axis=-1)[:, 0]
        tok_draft = jnp.take_along_axis(row_probs, row_tokens[:, None], axis=-1)[:, 0]
        accept = jnp.minimum(1.0, tok_target / tok_draft)
        excess = jnp.maximum(target - row_probs, 0.0)
        norm_sum = jnp.sum(excess, axis=-1)
        residual = excess / norm_sum[:, None]
        return accept, norm_sum, residual, row_lse[DRAFT_LEN, 0]

    accept, norm_sum, residual, bonus_lse = lax.map(one_row, (hidden, draft_probs, draft_tokens, temperature))
    return accept, norm_sum, residual, bonus_lse
```

```python
import functools

import jax
import jax.numpy as jnp
from jax import lax
from jax.experimental import pallas as pl
from jax.experimental.pallas import tpu as pltpu
from jax.sharding import PartitionSpec as P

LOG2E = 1.4426950408889634
LN2 = 0.6931471805599453
MESH = pl.DeviceIdType.MESH
TILE = 512
DEPTH = 9
GROUP = 3
Q_STEPS = 3
LOW = -3.0e38


def _verify_kernel(n, x_ref, k_ref, kp_ref, hit_ref, w_ref, q_ref, z_ref, stat_ref, norm_ref,
                   wbuf, wtail, qbuf, zt, m_ref, l_ref, lse_ref, send1, recv1, send2, recv2,
                   wsem, tsem, qsem, ssem1, rsem1, ssem2, rsem2):
    me = lax.axis_index('tp')
    dp = lax.axis_index('dp')
    vocab = w_ref.shape[0]
    width = w_ref.shape[1]
    rows = x_ref.shape[0]
    seqs = rows // 4
    draft_rows = rows - seqs
    groups = draft_rows // 8
    all_groups = rows // 8
    tiles = vocab // TILE
    tail = vocab - tiles * TILE
    tail_at = tiles * TILE
    lane = lax.broadcasted_iota(jnp.int32, (8, 128), 1)
    sub = lax.broadcasted_iota(jnp.int32, (8, 128), 0)

    def q_copy(g):
        at = pl.ds(pl.multiple_of(g * 8, 8), 8)
        return pltpu.make_async_copy(q_ref.at[at, :], qbuf.at[at, :], qsem.at[g])

    order = lambda r: lax.rem(r + tiles - 1, tiles)

    def w_copy(r):
        slot = lax.rem(r, DEPTH)
        at = pl.ds(pl.multiple_of(order(r) * TILE, TILE), TILE)
        return pltpu.make_async_copy(w_ref.at[at, :], wbuf.at[slot], wsem.at[slot])

    tail_copy = pltpu.make_async_copy(w_ref.at[pl.ds(tail_at, tail), :], wtail, tsem)
    tail_copy.start()
    for i in range(DEPTH):
        w_copy(i).start()

    barrier = pltpu.get_barrier_semaphore()
    for d in range(1, n):
        pl.semaphore_signal(barrier, inc=1, device_id=(dp, lax.rem(me + d, n)), device_id_type=MESH)

    m_ref[...] = jnp.full_like(m_ref, LOW)
    l_ref[...] = jnp.zeros_like(l_ref)

    def dot(w):
        return lax.dot_general(x_ref[...], w, (((1,), (1,)), ((), ())), preferred_element_type=jnp.float32)

    def process(src, tile):
        base = tile * TILE
        for g in range(all_groups):
            at = slice(g * 8, g * 8 + 8)
            k = k_ref[at, :]
            old = m_ref[at, :]
            parts = [src[at, c * 128:c * 128 + 128] for c in range(TILE // 128)]
            new = old
            for c, v in enumerate(parts):
                new = jnp.maximum(new, v)
                if g < groups:
                    z_ref[at, pl.ds(pl.multiple_of(base + c * 128, 128), 128)] = v
            total = l_ref[at, :] * jnp.exp2((old - new) * k)
            for v in parts:
                total = total + jnp.exp2((v - new) * k)
            m_ref[at, :] = new
            l_ref[at, :] = total

    def step(r, p, carry, refill=True):
        for t in range(GROUP):
            w_copy(r + t).wait()

        for t in range(GROUP if refill else 0):
            @pl.when(r - GROUP + t + DEPTH < tiles)
            def _():
                w_copy(r - GROUP + t + DEPTH).start()

        first = (r - 1) // GROUP - (steps - Q_STEPS)
        per = groups // Q_STEPS

        @pl.when(first >= 0)
        def _():
            for j in range(per):
                q_copy(first * per + j).start()

        for t in range(GROUP):
            zt[p, t] = dot(wbuf[lax.rem(r + t, DEPTH)])
            if t == 0:
                process(zt.at[1 - p, carry], order(r - 1))
            else:
                process(zt.at[p, t - 1], order(r + t - 1))

    steps = (tiles - 1) // GROUP
    tail_copy.wait()
    z_tail = dot(wtail[...])
    z_ref[:, tail_at:tail_at + tail] = z_tail[:draft_rows]
    m_ref[:, :tail] = z_tail
    l_ref[:, :tail] = jnp.ones_like(z_tail)
    w_copy(0).wait()
    zt[1, 0] = dot(wbuf[0])
    w_copy(DEPTH).start()

    step(1, 0, 0, refill=False)

    @pl.loop(0, (steps - 1) // 2)
    def _(t):
        r = 1 + GROUP * (1 + 2 * t)
        step(r, 1, GROUP - 1)
        step(r + GROUP, 0, GROUP - 1)

    last = 0
    if steps % 2 == 0:
        step(1 + GROUP * (steps - 1), 1, GROUP - 1)
        last = 1
    process(zt.at[last, GROUP - 1], order(tiles - 1))

    def pack(acc, g, col):
        return jnp.where((lane == g) | (lane == g + 32), col, acc)

    packed_m = jnp.zeros((8, 128), jnp.float32)
    packed_l = jnp.zeros((8, 128), jnp.float32)
    for g in range(all_groups):
        at = slice(g * 8, g * 8 + 8)
        m = m_ref[at, :]
        top = jnp.max(m, axis=1, keepdims=True)
        total = jnp.sum(l_ref[at, :] * jnp.exp2((m - top) * k_ref[at, :]), axis=1, keepdims=True)
        packed_m = pack(packed_m, g, top)
        packed_l = pack(packed_l, g, total)
    send1[0] = packed_m
    send1[1] = packed_l
    recv1[me, 0] = packed_m
    recv1[me, 1] = packed_l

    pl.semaphore_wait(barrier, n - 1)

    def share(src, dst, ssem, rsem):
        copies = []
        for d in range(1, n):
            copy = pltpu.make_async_remote_copy(
                src_ref=src, dst_ref=dst.at[me], send_sem=ssem.at[d], recv_sem=rsem.at[me],
                device_id=(dp, lax.rem(me + d, n)), device_id_type=MESH)
            copy.start()
            copies.append(copy)
        return copies

    def collect(src, dst, ssem, rsem):
        for d in range(1, n):
            peer = lax.rem(me + d, n)
            pltpu.make_async_remote_copy(
                src_ref=src, dst_ref=dst.at[peer], send_sem=ssem.at[d], recv_sem=rsem.at[peer],
                device_id=(dp, peer), device_id_type=MESH).wait_recv()

    copies1 = share(send1, recv1, ssem1, rsem1)

    def gather(ref, wait=None):
        def one(g, packed):
            if wait is not None:
                wait(g)
            at = pl.ds(pl.multiple_of(g * 8, 8), 8)
            hit = hit_ref[at, :]
            got = [jnp.zeros((8, 128), jnp.float32) for _ in range(4)]
            for c in range(vocab // 128):
                got[c % 4] = jnp.where(hit - c * 128 == lane, ref[at, c * 128:c * 128 + 128], got[c % 4])
            edge = (vocab // 128) * 128
            rest = vocab - edge
            last = jnp.where(hit[:, :rest] - edge == lane[:, :rest], ref[at, edge:], 0.0)
            col = jnp.sum((got[0] + got[1]) + (got[2] + got[3]), axis=1, keepdims=True)
            return pack(packed, g, col + jnp.sum(last, axis=1, keepdims=True))

        return lax.fori_loop(0, groups, one, jnp.zeros((8, 128), jnp.float32))

    tok_z = gather(z_ref)
    tok_q = gather(qbuf, lambda g: q_copy(g).wait())

    collect(send1, recv1, ssem1, rsem1)
    kp = kp_ref[...]
    top = recv1[0, 0]
    for i in range(1, n):
        top = jnp.maximum(top, recv1[i, 0])
    total = jnp.zeros((8, 128), jnp.float32)
    for i in range(n):
        total = total + recv1[i, 1] * jnp.exp2((recv1[i, 0] - top) * kp)
    lse = top * kp + jnp.log(total) * LOG2E
    stat_ref[1] = lse * LN2
    for g in range(groups):
        col = jnp.sum(jnp.where(lane == g, lse, 0.0), axis=1, keepdims=True)
        lse_ref[g * 8:g * 8 + 8, :] = jnp.broadcast_to(col, (8, 128))

    full = vocab // 128

    def excess(g, packed):
        at = pl.ds(pl.multiple_of(g * 8, 8), 8)
        k = k_ref[at, :]
        base = lse_ref[at, :]
        sums = [jnp.zeros((8, 128), jnp.float32) for _ in range(4)]
        for c in range(full):
            cols = slice(c * 128, c * 128 + 128)
            e = jnp.maximum(jnp.exp2(z_ref[at, cols] * k - base) - qbuf[at, cols], 0.0)
            z_ref[at, cols] = e
            sums[c % 4] = sums[c % 4] + e
        rest = vocab - full * 128
        cols = slice(full * 128, vocab)
        e = jnp.maximum(jnp.exp2(z_ref[at, cols] * k[:, :rest] - base[:, :rest]) - qbuf[at, cols], 0.0)
        z_ref[at, cols] = e
        col = jnp.sum((sums[0] + sums[1]) + (sums[2] + sums[3]), axis=1, keepdims=True)
        col = col + jnp.sum(e, axis=1, keepdims=True)
        return jnp.where(lane == g, col, packed)

    packed = lax.fori_loop(0, groups, excess, jnp.zeros((8, 128), jnp.float32))
    ones = jnp.where(tok_q > 0, tok_q, 1.0)
    accept = jnp.where(tok_q > 0, jnp.minimum(1.0, jnp.exp2(tok_z * kp - lse) / ones), 0.0)
    packed = jnp.where((lane >= 32) & (lane < 64), accept, packed)
    send2[...] = packed
    recv2[me] = packed
    copies2 = share(send2, recv2, ssem2, rsem2)
    collect(send2, recv2, ssem2, rsem2)
    total = recv2[0]
    for i in range(1, n):
        total = total + recv2[i]
    stat_ref[0] = total
    inv = 1.0 / total
    for g in range(groups):
        col = jnp.sum(jnp.where(lane == g, inv, 0.0), axis=1, keepdims=True)
        norm_ref[g * 8:g * 8 + 8, :] = jnp.broadcast_to(col, (8, 128))
    for copy in copies1 + copies2:
        copy.wait_send()


def _scale_kernel(e_ref, norm_ref, o_ref):
    rows, vocab = o_ref.shape
    step = pl.program_id(0)
    full = vocab // 128
    for g in range(rows // 8):
        at = pl.ds(pl.multiple_of(step * rows + g * 8, 8), 8)
        out = slice(g * 8, g * 8 + 8)
        inv = norm_ref[at, :]
        for c in range(full):
            cols = slice(c * 128, c * 128 + 128)
            o_ref[out, cols] = e_ref[at, cols] * inv
        cols = slice(full * 128, vocab)
        o_ref[out, cols] = e_ref[at, cols] * inv[:, :vocab - full * 128]


def solution(mesh):
    n = mesh.shape['tp']

    def local_step(hidden, norm_gain, w_head, draft_probs, draft_tokens, temperature):
        seqs, positions, width = hidden.shape
        vocab = w_head.shape[1]
        rows = seqs * positions
        draft = positions - 1
        draft_rows = seqs * draft
        h = hidden.astype(jnp.float32)
        inv_rms = lax.rsqrt(jnp.mean(h * h, axis=-1, keepdims=True) + 1e-5)
        x = (h * inv_rms * norm_gain).astype(jnp.bfloat16)
        x = x.transpose(1, 0, 2).reshape(rows, width)
        k = jnp.tile(LOG2E / temperature, positions)
        k_cols = jnp.broadcast_to(k[:, None], (rows, 128))
        kp = jnp.tile(k.reshape(rows // 8, 8).T, (1, 4))
        tok = draft_tokens.T.reshape(draft_rows) - lax.axis_index('tp') * vocab
        hit = jnp.where((tok >= 0) & (tok < vocab), tok, -1)
        hit = jnp.broadcast_to(hit[:, None], (draft_rows, 128))
        q = draft_probs.transpose(1, 0, 2).reshape(draft_rows, vocab)
        vmem = pl.BlockSpec(memory_space=pltpu.VMEM)
        hbm = pl.BlockSpec(memory_space=pl.ANY)
        f32 = jnp.float32
        z, stat, norm = pl.pallas_call(
            functools.partial(_verify_kernel, n),
            out_shape=(pltpu.VMEM((draft_rows, vocab), f32),
                       jax.ShapeDtypeStruct((2, 8, 128), f32),
                       pltpu.VMEM((draft_rows, 128), f32)),
            in_specs=[vmem, vmem, vmem, vmem, hbm, hbm],
            out_specs=(vmem, vmem, vmem),
            scratch_shapes=[
                pltpu.VMEM((DEPTH, TILE, width), jnp.bfloat16),
                pltpu.VMEM((vocab % TILE, width), jnp.bfloat16),
                pltpu.VMEM((draft_rows, vocab), f32),
                pltpu.VMEM((2, GROUP, rows, TILE), f32),
                pltpu.VMEM((rows, 128), f32),
                pltpu.VMEM((rows, 128), f32),
                pltpu.VMEM((draft_rows, 128), f32),
                pltpu.VMEM((2, 8, 128), f32),
                pltpu.VMEM((n, 2, 8, 128), f32),
                pltpu.VMEM((8, 128), f32),
                pltpu.VMEM((n, 8, 128), f32),
                pltpu.SemaphoreType.DMA((DEPTH,)),
                pltpu.SemaphoreType.DMA,
                pltpu.SemaphoreType.DMA((draft_rows // 8,)),
                pltpu.SemaphoreType.DMA((n,)),
                pltpu.SemaphoreType.DMA((n,)),
                pltpu.SemaphoreType.DMA((n,)),
                pltpu.SemaphoreType.DMA((n,)),
            ],
            compiler_params=pltpu.CompilerParams(
                collective_id=0, has_side_effects=True, vmem_limit_bytes=48 * 2**20),
            name='verify',
        )(x, k_cols, kp, hit, w_head.T, q)
        block = 16
        residual = pl.pallas_call(
            _scale_kernel,
            out_shape=jax.ShapeDtypeStruct((draft_rows, vocab), f32),
            grid=(draft_rows // block,),
            in_specs=[vmem, vmem],
            out_specs=pl.BlockSpec((block, vocab), lambda i: (i, 0)),
            compiler_params=pltpu.CompilerParams(vmem_limit_bytes=8 * 2**20),
            name='scale',
        )(z, norm)
        groups = draft_rows // 8
        norm_sum = stat[0, :, :groups].T.reshape(draft, seqs).T
        accept = stat[0, :, 32:32 + groups].T.reshape(draft, seqs).T
        bonus = stat[1, :, groups:rows // 8].T.reshape(seqs)
        return accept, norm_sum, residual.reshape(draft, seqs, vocab).transpose(1, 0, 2), bonus

    return jax.shard_map(
        local_step,
        mesh=mesh,
        in_specs=(P('dp', None, None), P(), P(None, 'tp'), P('dp', None, 'tp'), P('dp', None), P('dp')),
        out_specs=(P('dp', None), P('dp', None), P('dp', None, 'tp'), P('dp')),
        check_vma=False,
    )
```

```python
import functools

import jax
import jax.numpy as jnp
from jax import lax
from jax.experimental import pallas as pl
from jax.experimental.pallas import tpu as pltpu
from jax.sharding import PartitionSpec as P

LOG2E = 1.4426950408889634
LN2 = 0.6931471805599453
MESH = pl.DeviceIdType.MESH
TILE = 512
DEPTH = 10
LOW = -3.0e38


def _pack(packed, g, col):
    lane = lax.broadcasted_iota(jnp.int32, (8, 128), 1)
    return jnp.where((lane == g) | (lane == g + 32), col, packed)


def _stream_kernel(h_ref, gain_ref, temp_ref, tok_ref, w_ref,
                   z_ref, ml_ref, tok_z_ref, k_ref, kp_ref, hit_ref,
                   hbuf, gbuf, tbuf, dbuf, hp_ref, x_ref, tz_ref, wbuf, wtail, m_ref, l_ref,
                   wsem, tsem, isem):
    me = lax.axis_index('tp')
    vocab = w_ref.shape[0]
    width = w_ref.shape[1]
    seqs = h_ref.shape[0]
    rows = seqs * 4
    per = seqs // 8
    draft_rows = rows - seqs
    groups = draft_rows // 8
    all_groups = rows // 8
    tiles = vocab // TILE
    tail = vocab - tiles * TILE
    tail_at = tiles * TILE
    chunks = width // 256
    lane = lax.broadcasted_iota(jnp.int32, (8, 128), 1)
    sub = lax.broadcasted_iota(jnp.int32, (8, 128), 0)

    def w_copy(tile):
        slot = lax.rem(tile, DEPTH)
        return pltpu.make_async_copy(
            w_ref.at[pl.ds(pl.multiple_of(tile * TILE, TILE), TILE), :], wbuf.at[slot], wsem.at[slot])

    first_copies = [pltpu.make_async_copy(a, b, isem.at[i]) for i, (a, b) in enumerate(
        ((h_ref, hbuf), (temp_ref, tbuf), (gain_ref, gbuf), (tok_ref, dbuf)))]
    for copy in first_copies:
        copy.start()
    tail_copy = pltpu.make_async_copy(w_ref.at[pl.ds(tail_at, tail), :], wtail.at[pl.ds(0, tail), :], tsem)
    tail_copy.start()
    for i in range(DEPTH - 1):
        w_copy(i).start()

    m_ref[...] = jnp.full_like(m_ref, LOW)
    l_ref[...] = jnp.zeros_like(l_ref)
    tz_ref[...] = jnp.zeros_like(tz_ref)
    wtail[tail:, :] = jnp.zeros((wtail.shape[0] - tail, width), wtail.dtype)

    for copy in first_copies[1:]:
        copy.wait()

    def column(row, g):
        picked = jnp.where(lane[:, :seqs] == g * 8 + sub[:, :seqs], jnp.broadcast_to(row, (8, seqs)), 0.0)
        return jnp.sum(picked, axis=1, keepdims=True)

    kp = jnp.zeros((8, 128), jnp.float32)
    for g in range(per):
        k = jnp.broadcast_to(LOG2E / column(tbuf[...], g), (8, 128))
        k_ref[g * 8:g * 8 + 8, :] = k
        kp = jnp.where(lax.rem(lane, per) == g, k, kp)
    for j in range(3):
        row = (dbuf[j:j + 1, :] - me * vocab).astype(jnp.float32)
        for g in range(per):
            at = slice(j * seqs + g * 8, j * seqs + g * 8 + 8)
            hit_ref[at, :] = jnp.broadcast_to(column(row, g), (8, 128)).astype(jnp.int32)
    kp_ref[...] = kp
    first_copies[0].wait()

    def run(*accs):
        def acc(q, p, b):
            return accs[(q * 2 + p) * 4 + b]

        def accumulate(q, p, c):
            for b in range(4):
                pltpu.matmul_acc_lhs(
                    acc(q, p, b), x_ref[b * seqs:(b + 1) * seqs, c * 256:(c + 1) * 256],
                    load_staged_rhs=c % 2 if b == 0 else None)

        def push(tile, q, c):
            slot = lax.rem(tile, DEPTH)
            pltpu.matmul_push_rhs(
                wbuf[slot, q * 256:(q + 1) * 256, c * 256:(c + 1) * 256],
                staging_register=c % 2, mxu_index=q, transpose=True)

        cols = lax.broadcasted_iota(jnp.int32, (seqs, 128), 1)

        def update(b, parts, base):
            at = slice(b * seqs, (b + 1) * seqs)
            k = k_ref[...]
            old = m_ref[at, :]
            new = old
            if b < 3:
                hit = hit_ref[at, :] - base
                got = tz_ref[at, :]
                for i, v in enumerate(parts):
                    got = jnp.where(hit == cols + i * 128, v, got)
                tz_ref[at, :] = got
            for v in parts:
                new = jnp.maximum(new, v)
            total = l_ref[at, :] * jnp.exp2((old - new) * k)
            for v in parts:
                total = total + jnp.exp2((v - new) * k)
            m_ref[at, :] = new
            l_ref[at, :] = total

        def drain(tile, p, b):
            parts = []
            for q in range(2):
                v = pltpu.matmul_pop(acc(q, p, b))
                if b < 3:
                    at = pl.ds(pl.multiple_of(tile * TILE + q * 256, 256), 256)
                    z_ref[b * seqs:(b + 1) * seqs, at] = v
                parts += [v[:, :128], v[:, 128:]]
            update(b, parts, tile * TILE)

        def drain_tail(p, b):
            v = pltpu.matmul_pop(acc(0, p, b))
            if b < 3:
                z_ref[b * seqs:(b + 1) * seqs, tail_at:tail_at + tail] = v[:, :tail]
            update(b, [jnp.where(cols < tail, v[:, :128], LOW)], tail_at)

        def step(tile, p, last=False, first=False, refill=None):
            if not last:
                w_copy(tile + 1).wait()
            if refill is not None:
                refill()
            for c in range(chunks):
                for q in range(2):
                    accumulate(q, p, c)
                for q in range(2):
                    if c + 1 < chunks:
                        push(tile, q, c + 1)
                    elif not last:
                        push(tile + 1, q, 0)
                if 1 <= c <= 4:
                    if first:
                        drain_tail(1 - p, c - 1)
                    else:
                        drain(tile - 1, 1 - p, c - 1)

        c_of = lax.broadcasted_iota(jnp.int32, (seqs, 256), 1)
        r_of = lax.broadcasted_iota(jnp.int32, (seqs, 256), 0)
        for c in range(chunks):
            flat = hbuf[:, :, c * 256:(c + 1) * 256].reshape(rows, 256)
            pltpu.matmul_push_rhs(flat, staging_register=(c // 2) % 2, mxu_index=c % 2)
            for b in range(4):
                pick = jnp.where(c_of == r_of * 4 + b, 1.0, 0.0).astype(jnp.bfloat16)
                pltpu.matmul_acc_lhs(acc(c % 2, (c // 2) % 2, b), pick,
                                     load_staged_rhs=(c // 2) % 2 if b == 0 else None)
            for b in range(4):
                hp_ref[b * seqs:(b + 1) * seqs, c * 256:(c + 1) * 256] = pltpu.matmul_pop(acc(c % 2, (c // 2) % 2, b))
        gain = gbuf[...]
        for g in range(all_groups // 2):
            at = slice(g * 16, g * 16 + 16)
            h = hp_ref[at, :]
            inv_rms = lax.rsqrt(jnp.sum(h * h, axis=1, keepdims=True) * (1.0 / width) + 1e-5)
            x_ref[at, :] = (h * inv_rms * gain).astype(jnp.bfloat16)

        tail_copy.wait()
        for c in range(chunks):
            pltpu.matmul_push_rhs(wtail[:, c * 256:(c + 1) * 256], staging_register=c % 2, mxu_index=0, transpose=True)
            accumulate(0, 1, c)
        w_copy(0).wait()
        for q in range(2):
            push(0, q, 0)
        step(0, 0, first=True, refill=lambda: w_copy(DEPTH - 1).start())

        def refill_at(tile):
            @pl.when(tile + DEPTH - 1 < tiles)
            def _():
                w_copy(tile + DEPTH - 1).start()

        @pl.loop(0, (tiles - 3) // 2)
        def _(t):
            tile = 1 + 2 * t
            step(tile, 1, refill=lambda: refill_at(tile))
            step(tile + 1, 0, refill=lambda: refill_at(tile + 1))

        step(tiles - 2, 1)
        step(tiles - 1, 0, last=True)
        for b in range(4):
            drain(tiles - 1, 0, b)

    pl.run_scoped(run, *[pltpu.ACC(q)((seqs, 256), jnp.float32) for q in range(2) for _ in range(8)])

    packed_m = jnp.zeros((8, 128), jnp.float32)
    packed_l = jnp.zeros((8, 128), jnp.float32)
    tok_z = jnp.zeros((8, 128), jnp.float32)
    for g in range(all_groups):
        at = slice(g * 8, g * 8 + 8)
        m = m_ref[at, :]
        top = jnp.max(m, axis=1, keepdims=True)
        k = k_ref[g % per * 8:g % per * 8 + 8, :]
        total = jnp.sum(l_ref[at, :] * jnp.exp2((m - top) * k), axis=1, keepdims=True)
        packed_m = _pack(packed_m, g, top)
        packed_l = _pack(packed_l, g, total)
        if g < groups:
            tok_z = _pack(tok_z, g, jnp.sum(tz_ref[at, :], axis=1, keepdims=True))
    ml_ref[0] = packed_m
    ml_ref[1] = packed_l
    tok_z_ref[...] = tok_z


def _exchange_kernel(n, z_ref, ml_ref, tok_z_ref, k_ref, kp_ref, hit_ref, q_ref, e_ref, stat_ref, norm_ref,
                     lse_ref, recv1, send2, recv2, qsem, ssem1, rsem1, ssem2, rsem2):
    me = lax.axis_index('tp')
    dp = lax.axis_index('dp')
    draft_rows, vocab = q_ref.shape
    groups = draft_rows // 8
    per = k_ref.shape[0] // 8
    full = vocab // 128
    rest = vocab - full * 128
    edge = slice(full * 128, vocab)
    lane = lax.broadcasted_iota(jnp.int32, (8, 128), 1)

    def q_copy(g):
        at = pl.ds(pl.multiple_of(g * 8, 8), 8)
        return pltpu.make_async_copy(q_ref.at[at, :], e_ref.at[at, :], qsem.at[g])

    barrier = pltpu.get_barrier_semaphore()
    for d in range(1, n):
        pl.semaphore_signal(barrier, inc=1, device_id=(dp, lax.rem(me + d, n)), device_id_type=MESH)
    for g in range(groups):
        q_copy(g).start()
    recv1[me] = ml_ref[...]
    pl.semaphore_wait(barrier, n - 1)

    def share(src, dst, ssem, rsem):
        copies = []
        for d in range(1, n):
            copy = pltpu.make_async_remote_copy(
                src_ref=src, dst_ref=dst.at[me], send_sem=ssem.at[d], recv_sem=rsem.at[me],
                device_id=(dp, lax.rem(me + d, n)), device_id_type=MESH)
            copy.start()
            copies.append(copy)
        return copies

    def collect(src, dst, ssem, rsem):
        for d in range(1, n):
            peer = lax.rem(me + d, n)
            pltpu.make_async_remote_copy(
                src_ref=src, dst_ref=dst.at[peer], send_sem=ssem.at[d], recv_sem=rsem.at[peer],
                device_id=(dp, peer), device_id_type=MESH).wait_recv()

    copies1 = share(ml_ref, recv1, ssem1, rsem1)

    def gather(g, packed):
        q_copy(g).wait()
        at = pl.ds(pl.multiple_of(g * 8, 8), 8)
        hit = hit_ref[at, :]
        got = [jnp.zeros((8, 128), jnp.float32) for _ in range(4)]
        for c in range(full):
            got[c % 4] = jnp.where(hit - c * 128 == lane, e_ref[at, c * 128:c * 128 + 128], got[c % 4])
        last = jnp.where(hit[:, :rest] - full * 128 == lane[:, :rest], e_ref[at, edge], 0.0)
        col = jnp.sum((got[0] + got[1]) + (got[2] + got[3]), axis=1, keepdims=True)
        return _pack(packed, g, col + jnp.sum(last, axis=1, keepdims=True))

    tok_q = lax.fori_loop(0, groups, gather, jnp.zeros((8, 128), jnp.float32))

    collect(ml_ref, recv1, ssem1, rsem1)
    kp = kp_ref[...]
    top = recv1[0, 0]
    for i in range(1, n):
        top = jnp.maximum(top, recv1[i, 0])
    total = jnp.zeros((8, 128), jnp.float32)
    for i in range(n):
        total = total + recv1[i, 1] * jnp.exp2((recv1[i, 0] - top) * kp)
    lse = top * kp + jnp.log(total) * LOG2E
    stat_ref[1] = lse * LN2
    for g in range(groups):
        col = jnp.sum(jnp.where(lane == g, lse, 0.0), axis=1, keepdims=True)
        lse_ref[g * 8:g * 8 + 8, :] = jnp.broadcast_to(col, (8, 128))

    def excess(g, packed):
        at = pl.ds(pl.multiple_of(g * 8, 8), 8)
        k = k_ref[pl.ds(pl.multiple_of(lax.rem(g, per) * 8, 8), 8), :]
        base = lse_ref[at, :]
        sums = [jnp.zeros((8, 128), jnp.float32) for _ in range(4)]
        for c in range(full):
            cols = slice(c * 128, c * 128 + 128)
            e = jnp.maximum(jnp.exp2(z_ref[at, cols] * k - base) - e_ref[at, cols], 0.0)
            e_ref[at, cols] = e
            sums[c % 4] = sums[c % 4] + e
        e = jnp.maximum(jnp.exp2(z_ref[at, edge] * k[:, :rest] - base[:, :rest]) - e_ref[at, edge], 0.0)
        e_ref[at, edge] = e
        col = jnp.sum((sums[0] + sums[1]) + (sums[2] + sums[3]), axis=1, keepdims=True)
        col = col + jnp.sum(e, axis=1, keepdims=True)
        return jnp.where(lane == g, col, packed)

    packed = lax.fori_loop(0, groups, excess, jnp.zeros((8, 128), jnp.float32))
    below = jnp.where(tok_q > 0, tok_q, 1.0)
    accept = jnp.where(tok_q > 0, jnp.minimum(1.0, jnp.exp2(tok_z_ref[...] * kp - lse) / below), 0.0)
    packed = jnp.where((lane >= 32) & (lane < 64), accept, packed)
    send2[...] = packed
    recv2[me] = packed
    copies2 = share(send2, recv2, ssem2, rsem2)
    collect(send2, recv2, ssem2, rsem2)
    total = recv2[0]
    for i in range(1, n):
        total = total + recv2[i]
    stat_ref[0] = total
    inv = 1.0 / total
    for g in range(groups):
        col = jnp.sum(jnp.where(lane == g, inv, 0.0), axis=1, keepdims=True)
        norm_ref[g * 8:g * 8 + 8, :] = jnp.broadcast_to(col, (8, 128))
    for copy in copies1 + copies2:
        copy.wait_send()


def _scale_kernel(e_ref, norm_ref, stat_ref, o_ref, accept_ref, sum_ref, bonus_ref, stage, sem):
    rows, vocab = o_ref.shape
    full = vocab // 128
    slots = stage.shape[0]
    seqs = bonus_ref.shape[1]
    per = seqs // 8
    count = rows // 8

    def out_copy(g, slot):
        at = pl.ds(pl.multiple_of(g * 8, 8), 8)
        return pltpu.make_async_copy(stage.at[slot], o_ref.at[at, :], sem.at[slot])

    @pl.loop(0, count)
    def _(g):
        slot = lax.rem(g, slots)

        @pl.when(g >= slots)
        def _():
            out_copy(g - slots, slot).wait()

        at = pl.ds(pl.multiple_of(g * 8, 8), 8)
        inv = norm_ref[at, :]
        for c in range(full):
            cols = slice(c * 128, c * 128 + 128)
            stage[slot, :, cols] = e_ref[at, cols] * inv
        cols = slice(full * 128, vocab)
        stage[slot, :, cols] = e_ref[at, cols] * inv[:, :vocab - full * 128]
        out_copy(g, slot).start()

    lane = lax.broadcasted_iota(jnp.int32, (8, 128), 1)
    sub = lax.broadcasted_iota(jnp.int32, (8, 128), 0)

    def spread(packed, first):
        row = jnp.zeros((8, 128), jnp.float32)
        for g in range(per):
            col = jnp.sum(jnp.where(lane == first + g, packed, 0.0), axis=1, keepdims=True)
            row = jnp.where(lane == g * 8 + sub, col, row)
        return jnp.sum(row, axis=0, keepdims=True)[:, :seqs]

    for j in range(accept_ref.shape[0]):
        sum_ref[j:j + 1, :] = spread(stat_ref[0], j * per)
        accept_ref[j:j + 1, :] = spread(stat_ref[0], 32 + j * per)
    bonus_ref[...] = spread(stat_ref[1], count)
    for i in range(slots):
        out_copy(count - slots + i, lax.rem(count - slots + i, slots)).wait()


def solution(mesh):
    n = mesh.shape['tp']

    def local_step(hidden, norm_gain, w_head, draft_probs, draft_tokens, temperature):
        seqs, positions, width = hidden.shape
        vocab = w_head.shape[1]
        rows = seqs * positions
        draft = positions - 1
        draft_rows = seqs * draft
        q = draft_probs.transpose(1, 0, 2).reshape(draft_rows, vocab)
        vmem = pl.BlockSpec(memory_space=pltpu.VMEM)
        hbm = pl.BlockSpec(memory_space=pltpu.HBM)
        f32 = jnp.float32
        made = pl.pallas_call(
            _stream_kernel,
            out_shape=(pltpu.VMEM((draft_rows, vocab), f32),
                       pltpu.VMEM((2, 8, 128), f32),
                       pltpu.VMEM((8, 128), f32),
                       pltpu.VMEM((seqs, 128), f32),
                       pltpu.VMEM((8, 128), f32),
                       pltpu.VMEM((draft_rows, 128), jnp.int32)),
            in_specs=[hbm] * 5,
            out_specs=(vmem,) * 6,
            scratch_shapes=[
                pltpu.VMEM((seqs, positions, width), jnp.bfloat16),
                pltpu.VMEM((1, width), f32),
                pltpu.VMEM((1, seqs), f32),
                pltpu.VMEM((draft, seqs), jnp.int32),
                pltpu.VMEM((rows, width), f32),
                pltpu.VMEM((rows, width), jnp.bfloat16),
                pltpu.VMEM((draft_rows, 128), f32),
                pltpu.VMEM((DEPTH, TILE, width), jnp.bfloat16),
                pltpu.VMEM((256, width), jnp.bfloat16),
                pltpu.VMEM((rows, 128), f32),
                pltpu.VMEM((rows, 128), f32),
                pltpu.SemaphoreType.DMA((DEPTH,)),
                pltpu.SemaphoreType.DMA,
                pltpu.SemaphoreType.DMA((4,)),
            ],
            compiler_params=pltpu.CompilerParams(vmem_limit_bytes=28 * 2**20),
            name='stream',
        )(*[pltpu.with_memory_space_constraint(a, pltpu.HBM) for a in (
            hidden, norm_gain[None], temperature[None], draft_tokens.T, w_head.T)])
        z, stat, norm = pl.pallas_call(
            functools.partial(_exchange_kernel, n),
            out_shape=(pltpu.VMEM((draft_rows, vocab), f32),
                       pltpu.VMEM((2, 8, 128), f32),
                       pltpu.VMEM((draft_rows, 128), f32)),
            in_specs=[vmem] * 6 + [hbm],
            out_specs=(vmem,) * 3,
            scratch_shapes=[
                pltpu.VMEM((draft_rows, 128), f32),
                pltpu.VMEM((n, 2, 8, 128), f32),
                pltpu.VMEM((8, 128), f32),
                pltpu.VMEM((n, 8, 128), f32),
                pltpu.SemaphoreType.DMA((draft_rows // 8,)),
                pltpu.SemaphoreType.DMA((n,)),
                pltpu.SemaphoreType.DMA((n,)),
                pltpu.SemaphoreType.DMA((n,)),
                pltpu.SemaphoreType.DMA((n,)),
            ],
            compiler_params=pltpu.CompilerParams(
                collective_id=0, has_side_effects=True, vmem_limit_bytes=4 * 2**20),
            name='exchange',
        )(*[pltpu.with_memory_space_constraint(a, pltpu.VMEM) for a in made],
          pltpu.with_memory_space_constraint(q, pltpu.HBM))
        slots = 4
        residual, accept, norm_sum, bonus = pl.pallas_call(
            _scale_kernel,
            out_shape=(jax.ShapeDtypeStruct((draft_rows, vocab), f32),
                       jax.ShapeDtypeStruct((draft, seqs), f32),
                       jax.ShapeDtypeStruct((draft, seqs), f32),
                       jax.ShapeDtypeStruct((1, seqs), f32)),
            in_specs=[vmem, vmem, vmem],
            out_specs=(hbm, vmem, vmem, vmem),
            scratch_shapes=[pltpu.VMEM((slots, 8, vocab), f32), pltpu.SemaphoreType.DMA((slots,))],
            compiler_params=pltpu.CompilerParams(vmem_limit_bytes=8 * 2**20),
            name='scale',
        )(*[pltpu.with_memory_space_constraint(a, pltpu.VMEM) for a in (z, norm, stat)])
        residual = residual.reshape(draft, seqs, vocab).transpose(1, 0, 2)
        return accept.T, norm_sum.T, residual, bonus[0]

    return jax.shard_map(
        local_step,
        mesh=mesh,
        in_specs=(P('dp', None, None), P(), P(None, 'tp'), P('dp', None, 'tp'), P('dp', None), P('dp')),
        out_specs=(P('dp', None), P('dp', None), P('dp', None, 'tp'), P('dp')),
        check_vma=False,
    )
```

```python
import functools

import jax
import jax.numpy as jnp
from jax import lax
from jax.experimental import pallas as pl
from jax.experimental.pallas import tpu as pltpu
from jax.sharding import PartitionSpec as P

LOG2E = 1.4426950408889634
LN2 = 0.6931471805599453
MESH = pl.DeviceIdType.MESH
TILE = 512
DEPTH = 10
EARLY = 3
LOW = -3.0e38


def _pack(packed, g, col):
    lane = lax.broadcasted_iota(jnp.int32, (8, 128), 1)
    return jnp.where((lane == g) | (lane == g + 32), col, packed)


def _stream_kernel(h_ref, gain_ref, temp_ref, tok_ref, w_ref,
                   z_ref, ml_ref, k_ref, kp_ref, hit_ref,
                   hbuf, gbuf, tbuf, dbuf, hp_ref, x_ref, wbuf, wtail, m_ref, l_ref,
                   wsem, tsem, isem):
    me = lax.axis_index('tp')
    vocab = w_ref.shape[0]
    width = w_ref.shape[1]
    seqs = h_ref.shape[0]
    rows = seqs * 4
    per = seqs // 8
    draft_rows = rows - seqs
    groups = draft_rows // 8
    all_groups = rows // 8
    tiles = vocab // TILE
    tail = vocab - tiles * TILE
    tail_at = tiles * TILE
    chunks = width // 256
    lane = lax.broadcasted_iota(jnp.int32, (8, 128), 1)
    sub = lax.broadcasted_iota(jnp.int32, (8, 128), 0)

    def w_copy(tile):
        slot = lax.rem(tile, DEPTH)
        return pltpu.make_async_copy(
            w_ref.at[pl.ds(pl.multiple_of(tile * TILE, TILE), TILE), :], wbuf.at[slot], wsem.at[slot])

    first_copies = [pltpu.make_async_copy(a, b, isem.at[i]) for i, (a, b) in enumerate(
        ((h_ref, hbuf), (temp_ref, tbuf), (gain_ref, gbuf), (tok_ref, dbuf)))]
    for copy in first_copies:
        copy.start()
    tail_copy = pltpu.make_async_copy(w_ref.at[pl.ds(tail_at, tail), :], wtail.at[pl.ds(0, tail), :], tsem)
    tail_copy.start()
    for i in range(EARLY):
        w_copy(i).start()

    m_ref[...] = jnp.full_like(m_ref, LOW)
    l_ref[...] = jnp.zeros_like(l_ref)
    wtail[tail:, :] = jnp.zeros((wtail.shape[0] - tail, width), wtail.dtype)

    for copy in first_copies[1:]:
        copy.wait()

    def column(row, g):
        picked = jnp.where(lane[:, :seqs] == g * 8 + sub[:, :seqs], jnp.broadcast_to(row, (8, seqs)), 0.0)
        return jnp.sum(picked, axis=1, keepdims=True)

    kp = jnp.zeros((8, 128), jnp.float32)
    for g in range(per):
        k = jnp.broadcast_to(LOG2E / column(tbuf[...], g), (8, 128))
        k_ref[g * 8:g * 8 + 8, :] = k
        kp = jnp.where(lax.rem(lane, per) == g, k, kp)
    for j in range(3):
        row = (dbuf[j:j + 1, :] - me * vocab).astype(jnp.float32)
        for g in range(per):
            at = slice(j * seqs + g * 8, j * seqs + g * 8 + 8)
            hit_ref[at, :] = jnp.broadcast_to(column(row, g), (8, 128)).astype(jnp.int32)
    kp_ref[...] = kp
    first_copies[0].wait()
    for i in range(EARLY, DEPTH - 1):
        w_copy(i).start()

    def run(*accs):
        def acc(q, p, b):
            return accs[(q * 2 + p) * 4 + b]

        def accumulate(q, p, c):
            for b in range(4):
                pltpu.matmul_acc_lhs(
                    acc(q, p, b), x_ref[b * seqs:(b + 1) * seqs, c * 256:(c + 1) * 256],
                    load_staged_rhs=c % 2 if b == 0 else None)

        def push(tile, q, c):
            slot = lax.rem(tile, DEPTH)
            pltpu.matmul_push_rhs(
                wbuf[slot, q * 256:(q + 1) * 256, c * 256:(c + 1) * 256],
                staging_register=c % 2, mxu_index=q, transpose=True)

        cols = lax.broadcasted_iota(jnp.int32, (seqs, 128), 1)

        def update(b, parts):
            at = slice(b * seqs, (b + 1) * seqs)
            k = k_ref[...]
            old = m_ref[at, :]
            new = old
            for v in parts:
                new = jnp.maximum(new, v)
            total = l_ref[at, :] * jnp.exp2((old - new) * k)
            for v in parts:
                total = total + jnp.exp2((v - new) * k)
            m_ref[at, :] = new
            l_ref[at, :] = total

        def drain(tile, p, b):
            parts = []
            for q in range(2):
                v = pltpu.matmul_pop(acc(q, p, b))
                if b < 3:
                    at = pl.ds(pl.multiple_of(tile * TILE + q * 256, 256), 256)
                    z_ref[b * seqs:(b + 1) * seqs, at] = v
                parts += [v[:, :128], v[:, 128:]]
            update(b, parts)

        def drain_tail(p, b):
            v = pltpu.matmul_pop(acc(0, p, b))
            if b < 3:
                z_ref[b * seqs:(b + 1) * seqs, tail_at:tail_at + tail] = v[:, :tail]
            update(b, [jnp.where(cols < tail, v[:, :128], LOW)])

        def step(tile, p, last=False, first=False, refill=None):
            if not last:
                w_copy(tile + 1).wait()
            if refill is not None:
                refill()
            for c in range(chunks):
                for q in range(2):
                    accumulate(q, p, c)
                for q in range(2):
                    if c + 1 < chunks:
                        push(tile, q, c + 1)
                    elif not last:
                        push(tile + 1, q, 0)
                if 1 <= c <= 4:
                    if first:
                        drain_tail(1 - p, c - 1)
                    else:
                        drain(tile - 1, 1 - p, c - 1)

        c_of = lax.broadcasted_iota(jnp.int32, (seqs, 256), 1)
        r_of = lax.broadcasted_iota(jnp.int32, (seqs, 256), 0)
        for c in range(chunks):
            flat = hbuf[:, :, c * 256:(c + 1) * 256].reshape(rows, 256)
            pltpu.matmul_push_rhs(flat, staging_register=(c // 2) % 2, mxu_index=c % 2)
            for b in range(4):
                pick = jnp.where(c_of == r_of * 4 + b, 1.0, 0.0).astype(jnp.bfloat16)
                pltpu.matmul_acc_lhs(acc(c % 2, (c // 2) % 2, b), pick,
                                     load_staged_rhs=(c // 2) % 2 if b == 0 else None)
            for b in range(4):
                hp_ref[b * seqs:(b + 1) * seqs, c * 256:(c + 1) * 256] = pltpu.matmul_pop(acc(c % 2, (c // 2) % 2, b))
        gain = gbuf[...]
        for g in range(all_groups // 2):
            at = slice(g * 16, g * 16 + 16)
            h = hp_ref[at, :]
            inv_rms = lax.rsqrt(jnp.sum(h * h, axis=1, keepdims=True) * (1.0 / width) + 1e-5)
            for c in range(width // 128):
                cs = slice(c * 128, c * 128 + 128)
                x_ref[at, cs] = (h[:, cs] * inv_rms * gain[c:c + 1, :]).astype(jnp.bfloat16)

        tail_copy.wait()
        for c in range(chunks):
            pltpu.matmul_push_rhs(wtail[:, c * 256:(c + 1) * 256], staging_register=c % 2, mxu_index=0, transpose=True)
            accumulate(0, 1, c)
        w_copy(0).wait()
        for q in range(2):
            push(0, q, 0)
        step(0, 0, first=True, refill=lambda: w_copy(DEPTH - 1).start())

        def refill_at(tile):
            @pl.when(tile + DEPTH - 1 < tiles)
            def _():
                w_copy(tile + DEPTH - 1).start()

        @pl.loop(0, (tiles - 3) // 2)
        def _(t):
            tile = 1 + 2 * t
            step(tile, 1, refill=lambda: refill_at(tile))
            step(tile + 1, 0, refill=lambda: refill_at(tile + 1))

        step(tiles - 2, 1)
        step(tiles - 1, 0, last=True)
        for b in range(4):
            drain(tiles - 1, 0, b)

    pl.run_scoped(run, *[pltpu.ACC(q)((seqs, 256), jnp.float32) for q in range(2) for _ in range(8)])

    packed_m = jnp.zeros((8, 128), jnp.float32)
    packed_l = jnp.zeros((8, 128), jnp.float32)
    for g in range(all_groups):
        at = slice(g * 8, g * 8 + 8)
        m = m_ref[at, :]
        top = jnp.max(m, axis=1, keepdims=True)
        k = k_ref[g % per * 8:g % per * 8 + 8, :]
        total = jnp.sum(l_ref[at, :] * jnp.exp2((m - top) * k), axis=1, keepdims=True)
        packed_m = _pack(packed_m, g, top)
        packed_l = _pack(packed_l, g, total)
    ml_ref[0] = packed_m
    ml_ref[1] = packed_l


def _exchange_kernel(n, z_ref, ml_ref, k_ref, kp_ref, hit_ref, q_ref, e_ref, stat_ref, norm_ref,
                     lse_ref, part_q, part_z, recv1, send2, recv2, qsem, ssem1, rsem1, ssem2, rsem2):
    me = lax.axis_index('tp')
    dp = lax.axis_index('dp')
    draft_rows, vocab = q_ref.shape
    groups = draft_rows // 8
    per = k_ref.shape[0] // 8
    full = vocab // 128
    rest = vocab - full * 128
    edge = slice(full * 128, vocab)
    lane = lax.broadcasted_iota(jnp.int32, (8, 128), 1)

    def q_copy(g):
        at = pl.ds(pl.multiple_of(g * 8, 8), 8)
        return pltpu.make_async_copy(q_ref.at[at, :], e_ref.at[at, :], qsem.at[g])

    barrier = pltpu.get_barrier_semaphore()
    for d in range(1, n):
        pl.semaphore_signal(barrier, inc=1, device_id=(dp, lax.rem(me + d, n)), device_id_type=MESH)
    for g in range(groups):
        q_copy(g).start()
    recv1[me] = ml_ref[...]
    pl.semaphore_wait(barrier, n - 1)

    def share(src, dst, ssem, rsem):
        copies = []
        for d in range(1, n):
            copy = pltpu.make_async_remote_copy(
                src_ref=src, dst_ref=dst.at[me], send_sem=ssem.at[d], recv_sem=rsem.at[me],
                device_id=(dp, lax.rem(me + d, n)), device_id_type=MESH)
            copy.start()
            copies.append(copy)
        return copies

    def collect(src, dst, ssem, rsem):
        for d in range(1, n):
            peer = lax.rem(me + d, n)
            pltpu.make_async_remote_copy(
                src_ref=src, dst_ref=dst.at[peer], send_sem=ssem.at[d], recv_sem=rsem.at[peer],
                device_id=(dp, peer), device_id_type=MESH).wait_recv()

    copies1 = share(ml_ref, recv1, ssem1, rsem1)

    @pl.loop(0, groups)
    def _(g):
        q_copy(g).wait()
        at = pl.ds(pl.multiple_of(g * 8, 8), 8)
        hit = hit_ref[at, :]
        got_q = [jnp.zeros((8, 128), jnp.float32) for _ in range(2)]
        got_z = [jnp.zeros((8, 128), jnp.float32) for _ in range(2)]
        for c in range(full):
            cols = slice(c * 128, c * 128 + 128)
            here = hit - c * 128 == lane
            got_q[c % 2] = jnp.where(here, e_ref[at, cols], got_q[c % 2])
            got_z[c % 2] = jnp.where(here, z_ref[at, cols], got_z[c % 2])
        here = hit[:, :rest] - full * 128 == lane[:, :rest]
        part_q[at, :] = got_q[0] + got_q[1]
        part_z[at, :] = got_z[0] + got_z[1]
        part_q[at, :rest] = part_q[at, :rest] + jnp.where(here, e_ref[at, edge], 0.0)
        part_z[at, :rest] = part_z[at, :rest] + jnp.where(here, z_ref[at, edge], 0.0)

    tok_q = jnp.zeros((8, 128), jnp.float32)
    tok_z = jnp.zeros((8, 128), jnp.float32)
    for g in range(groups):
        at = slice(g * 8, g * 8 + 8)
        tok_q = _pack(tok_q, g, jnp.sum(part_q[at, :], axis=1, keepdims=True))
        tok_z = _pack(tok_z, g, jnp.sum(part_z[at, :], axis=1, keepdims=True))

    collect(ml_ref, recv1, ssem1, rsem1)
    kp = kp_ref[...]
    top = recv1[0, 0]
    for i in range(1, n):
        top = jnp.maximum(top, recv1[i, 0])
    total = jnp.zeros((8, 128), jnp.float32)
    for i in range(n):
        total = total + recv1[i, 1] * jnp.exp2((recv1[i, 0] - top) * kp)
    lse = top * kp + jnp.log(total) * LOG2E
    stat_ref[1] = lse * LN2
    for g in range(groups):
        col = jnp.sum(jnp.where(lane == g, lse, 0.0), axis=1, keepdims=True)
        lse_ref[g * 8:g * 8 + 8, :] = jnp.broadcast_to(col, (8, 128))

    def excess(g):
        at = pl.ds(pl.multiple_of(g * 8, 8), 8)
        k = k_ref[pl.ds(pl.multiple_of(lax.rem(g, per) * 8, 8), 8), :]
        base = lse_ref[at, :]
        sums = [jnp.zeros((8, 128), jnp.float32) for _ in range(4)]
        for c in range(full):
            cols = slice(c * 128, c * 128 + 128)
            e = jnp.maximum(jnp.exp2(z_ref[at, cols] * k - base) - e_ref[at, cols], 0.0)
            e_ref[at, cols] = e
            sums[c % 4] = sums[c % 4] + e
        e = jnp.maximum(jnp.exp2(z_ref[at, edge] * k[:, :rest] - base[:, :rest]) - e_ref[at, edge], 0.0)
        e_ref[at, edge] = e
        part_q[at, :] = (sums[0] + sums[1]) + (sums[2] + sums[3])
        part_q[at, :rest] = part_q[at, :rest] + e

    @pl.loop(0, groups // 2)
    def _(i):
        excess(2 * i)
        excess(2 * i + 1)

    packed = jnp.zeros((8, 128), jnp.float32)
    for g in range(groups):
        packed = _pack(packed, g, jnp.sum(part_q[g * 8:g * 8 + 8, :], axis=1, keepdims=True))
    below = jnp.where(tok_q > 0, tok_q, 1.0)
    accept = jnp.where(tok_q > 0, jnp.minimum(1.0, jnp.exp2(tok_z * kp - lse) / below), 0.0)
    packed = jnp.where((lane >= 32) & (lane < 64), accept, packed)
    send2[...] = packed
    recv2[me] = packed
    copies2 = share(send2, recv2, ssem2, rsem2)
    collect(send2, recv2, ssem2, rsem2)
    total = recv2[0]
    for i in range(1, n):
        total = total + recv2[i]
    stat_ref[0] = total
    inv = 1.0 / total
    for g in range(groups):
        col = jnp.sum(jnp.where(lane == g, inv, 0.0), axis=1, keepdims=True)
        norm_ref[g * 8:g * 8 + 8, :] = jnp.broadcast_to(col, (8, 128))
    for copy in copies1 + copies2:
        copy.wait_send()


def _scale_kernel(e_ref, norm_ref, stat_ref, o_ref, accept_ref, sum_ref, bonus_ref, stage, sem):
    rows, vocab = o_ref.shape
    full = vocab // 128
    slots = stage.shape[0]
    seqs = bonus_ref.shape[1]
    per = seqs // 8
    count = rows // 8

    def out_copy(g, slot):
        at = pl.ds(pl.multiple_of(g * 8, 8), 8)
        return pltpu.make_async_copy(stage.at[slot], o_ref.at[at, :], sem.at[slot])

    @pl.loop(0, count)
    def _(g):
        slot = lax.rem(g, slots)

        @pl.when(g >= slots)
        def _():
            out_copy(g - slots, slot).wait()

        at = pl.ds(pl.multiple_of(g * 8, 8), 8)
        inv = norm_ref[at, :]
        for c in range(full):
            cols = slice(c * 128, c * 128 + 128)
            stage[slot, :, cols] = e_ref[at, cols] * inv
        cols = slice(full * 128, vocab)
        stage[slot, :, cols] = e_ref[at, cols] * inv[:, :vocab - full * 128]
        out_copy(g, slot).start()

    lane = lax.broadcasted_iota(jnp.int32, (8, 128), 1)
    sub = lax.broadcasted_iota(jnp.int32, (8, 128), 0)

    def spread(packed, first):
        row = jnp.zeros((8, 128), jnp.float32)
        for g in range(per):
            col = jnp.sum(jnp.where(lane == first + g, packed, 0.0), axis=1, keepdims=True)
            row = jnp.where(lane == g * 8 + sub, col, row)
        return jnp.sum(row, axis=0, keepdims=True)[:, :seqs]

    for j in range(accept_ref.shape[0]):
        sum_ref[j:j + 1, :] = spread(stat_ref[0], j * per)
        accept_ref[j:j + 1, :] = spread(stat_ref[0], 32 + j * per)
    bonus_ref[...] = spread(stat_ref[1], count)
    for i in range(slots):
        out_copy(count - slots + i, lax.rem(count - slots + i, slots)).wait()


def solution(mesh):
    n = mesh.shape['tp']

    def local_step(hidden, norm_gain, w_head, draft_probs, draft_tokens, temperature):
        seqs, positions, width = hidden.shape
        vocab = w_head.shape[1]
        rows = seqs * positions
        draft = positions - 1
        draft_rows = seqs * draft
        q = draft_probs.transpose(1, 0, 2).reshape(draft_rows, vocab)
        vmem = pl.BlockSpec(memory_space=pltpu.VMEM)
        hbm = pl.BlockSpec(memory_space=pltpu.HBM)
        f32 = jnp.float32
        made = pl.pallas_call(
            _stream_kernel,
            out_shape=(pltpu.VMEM((draft_rows, vocab), f32),
                       pltpu.VMEM((2, 8, 128), f32),
                       pltpu.VMEM((seqs, 128), f32),
                       pltpu.VMEM((8, 128), f32),
                       pltpu.VMEM((draft_rows, 128), jnp.int32)),
            in_specs=[hbm] * 5,
            out_specs=(vmem,) * 5,
            scratch_shapes=[
                pltpu.VMEM((seqs, positions, width), jnp.bfloat16),
                pltpu.VMEM((width // 128, 128), f32),
                pltpu.VMEM((1, seqs), f32),
                pltpu.VMEM((draft, seqs), jnp.int32),
                pltpu.VMEM((rows, width), f32),
                pltpu.VMEM((rows, width), jnp.bfloat16),
                pltpu.VMEM((DEPTH, TILE, width), jnp.bfloat16),
                pltpu.VMEM((256, width), jnp.bfloat16),
                pltpu.VMEM((rows, 128), f32),
                pltpu.VMEM((rows, 128), f32),
                pltpu.SemaphoreType.DMA((DEPTH,)),
                pltpu.SemaphoreType.DMA,
                pltpu.SemaphoreType.DMA((4,)),
            ],
            compiler_params=pltpu.CompilerParams(vmem_limit_bytes=28 * 2**20),
            name='stream',
        )(*[pltpu.with_memory_space_constraint(a, pltpu.HBM) for a in (
            hidden, norm_gain.reshape(width // 128, 128), temperature[None], draft_tokens.T, w_head.T)])
        z, stat, norm = pl.pallas_call(
            functools.partial(_exchange_kernel, n),
            out_shape=(pltpu.VMEM((draft_rows, vocab), f32),
                       pltpu.VMEM((2, 8, 128), f32),
                       pltpu.VMEM((draft_rows, 128), f32)),
            in_specs=[vmem] * 5 + [hbm],
            out_specs=(vmem,) * 3,
            scratch_shapes=[
                pltpu.VMEM((draft_rows, 128), f32),
                pltpu.VMEM((draft_rows, 128), f32),
                pltpu.VMEM((draft_rows, 128), f32),
                pltpu.VMEM((n, 2, 8, 128), f32),
                pltpu.VMEM((8, 128), f32),
                pltpu.VMEM((n, 8, 128), f32),
                pltpu.SemaphoreType.DMA((draft_rows // 8,)),
                pltpu.SemaphoreType.DMA((n,)),
                pltpu.SemaphoreType.DMA((n,)),
                pltpu.SemaphoreType.DMA((n,)),
                pltpu.SemaphoreType.DMA((n,)),
            ],
            compiler_params=pltpu.CompilerParams(
                collective_id=0, has_side_effects=True, vmem_limit_bytes=8 * 2**20),
            name='exchange',
        )(*[pltpu.with_memory_space_constraint(a, pltpu.VMEM) for a in made],
          pltpu.with_memory_space_constraint(q, pltpu.HBM))
        slots = 8
        residual, accept, norm_sum, bonus = pl.pallas_call(
            _scale_kernel,
            out_shape=(jax.ShapeDtypeStruct((draft_rows, vocab), f32),
                       jax.ShapeDtypeStruct((draft, seqs), f32),
                       jax.ShapeDtypeStruct((draft, seqs), f32),
                       jax.ShapeDtypeStruct((1, seqs), f32)),
            in_specs=[vmem, vmem, vmem],
            out_specs=(hbm, vmem, vmem, vmem),
            scratch_shapes=[pltpu.VMEM((slots, 8, vocab), f32), pltpu.SemaphoreType.DMA((slots,))],
            compiler_params=pltpu.CompilerParams(vmem_limit_bytes=8 * 2**20),
            name='scale',
        )(*[pltpu.with_memory_space_constraint(a, pltpu.VMEM) for a in (z, norm, stat)])
        residual = residual.reshape(draft, seqs, vocab).transpose(1, 0, 2)
        return accept.T, norm_sum.T, residual, bonus[0]

    return jax.shard_map(
        local_step,
        mesh=mesh,
        in_specs=(P('dp', None, None), P(), P(None, 'tp'), P('dp', None, 'tp'), P('dp', None), P('dp')),
        out_specs=(P('dp', None), P('dp', None), P('dp', None, 'tp'), P('dp')),
        check_vma=False,
    )
```

```python
import functools

import jax
import jax.numpy as jnp
from jax import lax
from jax.experimental import pallas as pl
from jax.experimental.pallas import tpu as pltpu
from jax.sharding import PartitionSpec as P

LOG2E = 1.4426950408889634
LN2 = 0.6931471805599453
MESH = pl.DeviceIdType.MESH
TILE = 512
DEPTH = 8
EARLY = 2
LOW = -3.0e38


def _pack(packed, g, col):
    lane = lax.broadcasted_iota(jnp.int32, (8, 128), 1)
    return jnp.where((lane == g) | (lane == g + 32), col, packed)


def _stream_kernel(h_ref, gain_ref, temp_ref, tok_ref, w_ref,
                   z_ref, ml_ref, k_ref, mk_ref, kp_ref, hit_ref,
                   hbuf, gbuf, tbuf, dbuf, hp_ref, x_ref, wbuf, wtail, m_ref, l_ref,
                   wsem, tsem, isem):
    me = lax.axis_index('tp')
    vocab = w_ref.shape[0]
    width = w_ref.shape[1]
    seqs = h_ref.shape[0]
    rows = seqs * 4
    per = seqs // 8
    draft_rows = rows - seqs
    groups = draft_rows // 8
    all_groups = rows // 8
    tiles = vocab // TILE
    tail = vocab - tiles * TILE
    tail_at = tiles * TILE
    chunks = width // 256
    lane = lax.broadcasted_iota(jnp.int32, (8, 128), 1)
    sub = lax.broadcasted_iota(jnp.int32, (8, 128), 0)

    def w_copy(tile):
        slot = lax.rem(tile, DEPTH)
        return pltpu.make_async_copy(
            w_ref.at[pl.ds(pl.multiple_of(tile * TILE, TILE), TILE), :], wbuf.at[slot], wsem.at[slot])

    first_copies = [pltpu.make_async_copy(a, b, isem.at[i]) for i, (a, b) in enumerate(
        ((h_ref, hbuf), (temp_ref, tbuf), (gain_ref, gbuf), (tok_ref, dbuf)))]
    for copy in first_copies:
        copy.start()
    tail_copy = pltpu.make_async_copy(w_ref.at[pl.ds(tail_at, tail), :], wtail.at[pl.ds(0, tail), :], tsem)
    tail_copy.start()
    for i in range(EARLY):
        w_copy(i).start()

    m_ref[...] = jnp.full_like(m_ref, LOW)
    l_ref[...] = jnp.zeros_like(l_ref)
    wtail[tail:, :] = jnp.zeros((wtail.shape[0] - tail, width), wtail.dtype)

    for copy in first_copies[1:]:
        copy.wait()

    def column(row, g):
        picked = jnp.where(lane[:, :seqs] == g * 8 + sub[:, :seqs], jnp.broadcast_to(row, (8, seqs)), 0.0)
        return jnp.sum(picked, axis=1, keepdims=True)

    kp = jnp.zeros((8, 128), jnp.float32)
    for g in range(per):
        k = jnp.broadcast_to(LOG2E / column(tbuf[...], g), (8, 128))
        k_ref[g * 8:g * 8 + 8, :] = k
        kp = jnp.where(lax.rem(lane, per) == g, k, kp)
    for j in range(3):
        row = (dbuf[j:j + 1, :] - me * vocab).astype(jnp.float32)
        for g in range(per):
            at = slice(j * seqs + g * 8, j * seqs + g * 8 + 8)
            hit_ref[at, :] = jnp.broadcast_to(column(row, g), (8, 128)).astype(jnp.int32)
    kp_ref[...] = kp
    first_copies[0].wait()
    for i in range(EARLY, DEPTH - 1):
        w_copy(i).start()

    def run(*accs):
        def acc(q, p, b):
            return accs[(q * 2 + p) * 4 + b]

        def accumulate(q, p, c, staged=None):
            staged = c % 2 if staged is None else staged
            for b in range(4):
                pltpu.matmul_acc_lhs(
                    acc(q, p, b), x_ref[b * seqs:(b + 1) * seqs, c * 256:(c + 1) * 256],
                    load_staged_rhs=staged if b == 0 else None)

        def push(tile, q, c):
            slot = lax.rem(tile, DEPTH)
            pltpu.matmul_push_rhs(
                wbuf[slot, q * 256:(q + 1) * 256, c * 256:(c + 1) * 256],
                staging_register=c % 2, mxu_index=q, transpose=True)

        cols = lax.broadcasted_iota(jnp.int32, (seqs, 128), 1)

        def update(b, parts):
            at = slice(b * seqs, (b + 1) * seqs)
            k = k_ref[...]
            old = m_ref[at, :]
            new = old
            for v in parts:
                new = jnp.maximum(new, v)
            total = l_ref[at, :] * jnp.exp2((old - new) * k)
            for v in parts:
                total = total + jnp.exp2((v - new) * k)
            m_ref[at, :] = new
            l_ref[at, :] = total

        def drain(tile, p, b):
            parts = []
            for q in range(2):
                v = pltpu.matmul_pop(acc(q, p, b))
                if b < 3:
                    at = pl.ds(pl.multiple_of(tile * TILE + q * 256, 256), 256)
                    z_ref[b * seqs:(b + 1) * seqs, at] = v
                parts += [v[:, :128], v[:, 128:]]
            update(b, parts)

        def drain_tail(p, b):
            v = pltpu.matmul_pop(acc(0, p, b)) + pltpu.matmul_pop(acc(1, p, b))
            if b < 3:
                z_ref[b * seqs:(b + 1) * seqs, tail_at:tail_at + tail] = v[:, :tail]
            update(b, [jnp.where(cols < tail, v[:, :128], LOW)])

        def step(tile, p, last=False, first=False, refill=None):
            if not last:
                w_copy(tile + 1).wait()
            if refill is not None:
                refill()
            for c in range(chunks):
                for q in range(2):
                    accumulate(q, p, c)
                for q in range(2):
                    if c + 1 < chunks:
                        push(tile, q, c + 1)
                    elif not last:
                        push(tile + 1, q, 0)
                if 1 <= c <= 4:
                    if first:
                        drain_tail(1 - p, c - 1)
                    else:
                        drain(tile - 1, 1 - p, c - 1)

        c_of = lax.broadcasted_iota(jnp.int32, (seqs, 256), 1)
        r_of = lax.broadcasted_iota(jnp.int32, (seqs, 256), 0)
        def reorder(c):
            flat = hbuf[:, :, c * 256:(c + 1) * 256].reshape(rows, 256)
            pltpu.matmul_push_rhs(flat, staging_register=(c // 2) % 2, mxu_index=c % 2)
            for b in range(4):
                pick = jnp.where(c_of == r_of * 4 + b, 1.0, 0.0).astype(jnp.bfloat16)
                pltpu.matmul_acc_lhs(acc(c % 2, (c // 2) % 2, b), pick,
                                     load_staged_rhs=(c // 2) % 2 if b == 0 else None)

        def reordered(c):
            for b in range(4):
                hp_ref[b * seqs:(b + 1) * seqs, c * 256:(c + 1) * 256] = pltpu.matmul_pop(acc(c % 2, (c // 2) % 2, b))

        for c in range(chunks):
            if c >= 4:
                reordered(c - 4)
            reorder(c)
        for c in range(max(0, chunks - 4), chunks):
            reordered(c)
        gain = gbuf[...]
        for g in range(all_groups // 2):
            at = slice(g * 16, g * 16 + 16)
            h = hp_ref[at, :]
            inv_rms = lax.rsqrt(jnp.sum(h * h, axis=1, keepdims=True) * (1.0 / width) + 1e-5)
            for c in range(width // 128):
                cs = slice(c * 128, c * 128 + 128)
                x_ref[at, cs] = (h[:, cs] * inv_rms * gain[c:c + 1, :]).astype(jnp.bfloat16)

        tail_copy.wait()
        half = chunks // 2
        for i in range(half):
            for q in range(2):
                c = q * half + i
                pltpu.matmul_push_rhs(wtail[:, c * 256:(c + 1) * 256], staging_register=i % 2, mxu_index=q, transpose=True)
                accumulate(q, 1, c, i % 2)
        w_copy(0).wait()
        for q in range(2):
            push(0, q, 0)
        step(0, 0, first=True, refill=lambda: w_copy(DEPTH - 1).start())

        def refill_at(tile):
            @pl.when(tile + DEPTH - 1 < tiles)
            def _():
                w_copy(tile + DEPTH - 1).start()

        @pl.loop(0, (tiles - 3) // 2)
        def _(t):
            tile = 1 + 2 * t
            step(tile, 1, refill=lambda: refill_at(tile))
            step(tile + 1, 0, refill=lambda: refill_at(tile + 1))

        step(tiles - 2, 1)
        step(tiles - 1, 0, last=True)
        for b in range(4):
            drain(tiles - 1, 0, b)

    pl.run_scoped(run, *[pltpu.ACC(q)((seqs, 256), jnp.float32) for q in range(2) for _ in range(8)])

    packed_m = jnp.zeros((8, 128), jnp.float32)
    packed_l = jnp.zeros((8, 128), jnp.float32)
    for g in range(all_groups):
        at = slice(g * 8, g * 8 + 8)
        m = m_ref[at, :]
        top = jnp.max(m, axis=1, keepdims=True)
        k = k_ref[g % per * 8:g % per * 8 + 8, :]
        total = jnp.sum(l_ref[at, :] * jnp.exp2((m - top) * k), axis=1, keepdims=True)
        packed_m = _pack(packed_m, g, top)
        if g < groups:
            mk_ref[at, :] = top * k
        packed_l = _pack(packed_l, g, total)
    ml_ref[0] = packed_m
    ml_ref[1] = packed_l


def _exchange_kernel(n, z_ref, ml_ref, k_ref, mk_ref, kp_ref, hit_ref, q_ref, e_ref, stat_ref, norm_ref,
                     y_ref, scale_ref, part_q, part_z, recv1, send2, recv2, qsem, ssem1, rsem1, ssem2, rsem2):
    me = lax.axis_index('tp')
    dp = lax.axis_index('dp')
    draft_rows, vocab = q_ref.shape
    groups = draft_rows // 8
    per = k_ref.shape[0] // 8
    full = vocab // 128
    rest = vocab - full * 128
    edge = slice(full * 128, vocab)
    lane = lax.broadcasted_iota(jnp.int32, (8, 128), 1)

    def q_copy(g):
        at = pl.ds(pl.multiple_of(g * 8, 8), 8)
        return pltpu.make_async_copy(q_ref.at[at, :], e_ref.at[at, :], qsem.at[g])

    barrier = pltpu.get_barrier_semaphore()
    for d in range(1, n):
        pl.semaphore_signal(barrier, inc=1, device_id=(dp, lax.rem(me + d, n)), device_id_type=MESH)
    for g in range(groups):
        q_copy(g).start()
    recv1[me] = ml_ref[...]
    pl.semaphore_wait(barrier, n - 1)

    def share(src, dst, ssem, rsem):
        copies = []
        for d in range(1, n):
            copy = pltpu.make_async_remote_copy(
                src_ref=src, dst_ref=dst.at[me], send_sem=ssem.at[d], recv_sem=rsem.at[me],
                device_id=(dp, lax.rem(me + d, n)), device_id_type=MESH)
            copy.start()
            copies.append(copy)
        return copies

    def collect(src, dst, ssem, rsem):
        for d in range(1, n):
            peer = lax.rem(me + d, n)
            pltpu.make_async_remote_copy(
                src_ref=src, dst_ref=dst.at[peer], send_sem=ssem.at[d], recv_sem=rsem.at[peer],
                device_id=(dp, peer), device_id_type=MESH).wait_recv()

    copies1 = share(ml_ref, recv1, ssem1, rsem1)

    @pl.loop(0, groups)
    def _(g):
        q_copy(g).wait()
        at = pl.ds(pl.multiple_of(g * 8, 8), 8)
        hit = hit_ref[at, :]
        k = k_ref[pl.ds(pl.multiple_of(lax.rem(g, per) * 8, 8), 8), :]
        mk = mk_ref[at, :]
        got_q = [jnp.zeros((8, 128), jnp.float32) for _ in range(2)]
        got_z = [jnp.zeros((8, 128), jnp.float32) for _ in range(2)]
        for c in range(full):
            cols = slice(c * 128, c * 128 + 128)
            here = hit - c * 128 == lane
            z = z_ref[at, cols]
            y_ref[at, cols] = jnp.exp2(z * k - mk)
            got_q[c % 2] = jnp.where(here, e_ref[at, cols], got_q[c % 2])
            got_z[c % 2] = jnp.where(here, z, got_z[c % 2])
        y_ref[at, edge] = jnp.exp2(z_ref[at, edge] * k[:, :rest] - mk[:, :rest])
        here = hit[:, :rest] - full * 128 == lane[:, :rest]
        part_q[at, :] = got_q[0] + got_q[1]
        part_z[at, :] = got_z[0] + got_z[1]
        part_q[at, :rest] = part_q[at, :rest] + jnp.where(here, e_ref[at, edge], 0.0)
        part_z[at, :rest] = part_z[at, :rest] + jnp.where(here, z_ref[at, edge], 0.0)

    tok_q = jnp.zeros((8, 128), jnp.float32)
    tok_z = jnp.zeros((8, 128), jnp.float32)
    for g in range(groups):
        at = slice(g * 8, g * 8 + 8)
        tok_q = _pack(tok_q, g, jnp.sum(part_q[at, :], axis=1, keepdims=True))
        tok_z = _pack(tok_z, g, jnp.sum(part_z[at, :], axis=1, keepdims=True))

    collect(ml_ref, recv1, ssem1, rsem1)
    kp = kp_ref[...]
    top = recv1[0, 0]
    for i in range(1, n):
        top = jnp.maximum(top, recv1[i, 0])
    total = jnp.zeros((8, 128), jnp.float32)
    for i in range(n):
        total = total + recv1[i, 1] * jnp.exp2((recv1[i, 0] - top) * kp)
    lse = top * kp + jnp.log(total) * LOG2E
    stat_ref[1] = lse * LN2
    for g in range(groups):
        col = jnp.sum(jnp.where(lane == g, lse, 0.0), axis=1, keepdims=True)
        scale_ref[g * 8:g * 8 + 8, :] = jnp.exp2(mk_ref[g * 8:g * 8 + 8, :] - col)

    def excess(g):
        at = pl.ds(pl.multiple_of(g * 8, 8), 8)
        base = scale_ref[at, :]
        sums = [jnp.zeros((8, 128), jnp.float32) for _ in range(4)]
        for c in range(full):
            cols = slice(c * 128, c * 128 + 128)
            e = jnp.maximum(y_ref[at, cols] * base - e_ref[at, cols], 0.0)
            e_ref[at, cols] = e
            sums[c % 4] = sums[c % 4] + e
        e = jnp.maximum(y_ref[at, edge] * base[:, :rest] - e_ref[at, edge], 0.0)
        e_ref[at, edge] = e
        part_q[at, :] = (sums[0] + sums[1]) + (sums[2] + sums[3])
        part_q[at, :rest] = part_q[at, :rest] + e

    @pl.loop(0, groups // 2)
    def _(i):
        excess(2 * i)
        excess(2 * i + 1)

    packed = jnp.zeros((8, 128), jnp.float32)
    for g in range(groups):
        packed = _pack(packed, g, jnp.sum(part_q[g * 8:g * 8 + 8, :], axis=1, keepdims=True))
    below = jnp.where(tok_q > 0, tok_q, 1.0)
    accept = jnp.where(tok_q > 0, jnp.minimum(1.0, jnp.exp2(tok_z * kp - lse) / below), 0.0)
    packed = jnp.where((lane >= 32) & (lane < 64), accept, packed)
    send2[...] = packed
    recv2[me] = packed
    copies2 = share(send2, recv2, ssem2, rsem2)
    collect(send2, recv2, ssem2, rsem2)
    total = recv2[0]
    for i in range(1, n):
        total = total + recv2[i]
    stat_ref[0] = total
    inv = 1.0 / total
    for g in range(groups):
        col = jnp.sum(jnp.where(lane == g, inv, 0.0), axis=1, keepdims=True)
        norm_ref[g * 8:g * 8 + 8, :] = jnp.broadcast_to(col, (8, 128))
    for copy in copies1 + copies2:
        copy.wait_send()


def _scale_kernel(e_ref, norm_ref, stat_ref, o_ref, accept_ref, sum_ref, bonus_ref, stage, small, sem, ssem):
    rows, vocab = o_ref.shape
    full = vocab // 128
    slots = stage.shape[0]
    seqs = bonus_ref.shape[1]
    per = seqs // 8
    count = rows // 8

    def out_copy(g, slot):
        at = pl.ds(pl.multiple_of(g * 8, 8), 8)
        return pltpu.make_async_copy(stage.at[slot], o_ref.at[at, :], sem.at[slot])

    def scale(g):
        slot = lax.rem(g, slots)
        at = pl.ds(pl.multiple_of(g * 8, 8), 8)
        inv = norm_ref[at, :]
        for c in range(full):
            cols = slice(c * 128, c * 128 + 128)
            stage[slot, :, cols] = e_ref[at, cols] * inv
        cols = slice(full * 128, vocab)
        stage[slot, :, cols] = e_ref[at, cols] * inv[:, :vocab - full * 128]
        out_copy(g, slot).start()

    @pl.loop(0, slots)
    def _(g):
        scale(g)

    lane = lax.broadcasted_iota(jnp.int32, (8, 128), 1)
    sub = lax.broadcasted_iota(jnp.int32, (8, 128), 0)

    def spread(packed, first):
        row = jnp.zeros((8, 128), jnp.float32)
        for g in range(per):
            col = jnp.sum(jnp.where(lane == first + g, packed, 0.0), axis=1, keepdims=True)
            row = jnp.where(lane == g * 8 + sub, col, row)
        return jnp.sum(row, axis=0, keepdims=True)[:, :seqs]

    draft = accept_ref.shape[0]
    for j in range(draft):
        small[0, j:j + 1, :] = spread(stat_ref[0], 32 + j * per)
        small[1, j:j + 1, :] = spread(stat_ref[0], j * per)
    small[2, 0:1, :] = spread(stat_ref[1], count)
    smalls = [pltpu.make_async_copy(small.at[0, pl.ds(0, draft), :], accept_ref, ssem.at[0]),
              pltpu.make_async_copy(small.at[1, pl.ds(0, draft), :], sum_ref, ssem.at[1]),
              pltpu.make_async_copy(small.at[2, pl.ds(0, 1), :], bonus_ref, ssem.at[2])]

    @pl.loop(slots, count)
    def _(g):
        out_copy(g - slots, lax.rem(g, slots)).wait()
        scale(g)

        @pl.when(g == slots)
        def _():
            for copy in smalls:
                copy.start()

    for copy in smalls:
        copy.wait()
    for i in range(slots):
        out_copy(count - slots + i, lax.rem(count - slots + i, slots)).wait()


def solution(mesh):
    n = mesh.shape['tp']

    def local_step(hidden, norm_gain, w_head, draft_probs, draft_tokens, temperature):
        seqs, positions, width = hidden.shape
        vocab = w_head.shape[1]
        rows = seqs * positions
        draft = positions - 1
        draft_rows = seqs * draft
        q = draft_probs.transpose(1, 0, 2).reshape(draft_rows, vocab)
        vmem = pl.BlockSpec(memory_space=pltpu.VMEM)
        hbm = pl.BlockSpec(memory_space=pltpu.HBM)
        f32 = jnp.float32
        made = pl.pallas_call(
            _stream_kernel,
            out_shape=(pltpu.VMEM((draft_rows, vocab), f32),
                       pltpu.VMEM((2, 8, 128), f32),
                       pltpu.VMEM((seqs, 128), f32),
                       pltpu.VMEM((draft_rows, 128), f32),
                       pltpu.VMEM((8, 128), f32),
                       pltpu.VMEM((draft_rows, 128), jnp.int32)),
            in_specs=[hbm] * 5,
            out_specs=(vmem,) * 6,
            scratch_shapes=[
                pltpu.VMEM((seqs, positions, width), jnp.bfloat16),
                pltpu.VMEM((width // 128, 128), f32),
                pltpu.VMEM((1, seqs), f32),
                pltpu.VMEM((draft, seqs), jnp.int32),
                pltpu.VMEM((rows, width), f32),
                pltpu.VMEM((rows, width), jnp.bfloat16),
                pltpu.VMEM((DEPTH, TILE, width), jnp.bfloat16),
                pltpu.VMEM((256, width), jnp.bfloat16),
                pltpu.VMEM((rows, 128), f32),
                pltpu.VMEM((rows, 128), f32),
                pltpu.SemaphoreType.DMA((DEPTH,)),
                pltpu.SemaphoreType.DMA,
                pltpu.SemaphoreType.DMA((4,)),
            ],
            compiler_params=pltpu.CompilerParams(vmem_limit_bytes=28 * 2**20),
            name='stream',
        )(*[pltpu.with_memory_space_constraint(a, pltpu.HBM) for a in (
            hidden, norm_gain.reshape(width // 128, 128), temperature[None], draft_tokens.T, w_head.T)])
        z, stat, norm = pl.pallas_call(
            functools.partial(_exchange_kernel, n),
            out_shape=(pltpu.VMEM((draft_rows, vocab), f32),
                       pltpu.VMEM((2, 8, 128), f32),
                       pltpu.VMEM((draft_rows, 128), f32)),
            in_specs=[vmem] * 6 + [hbm],
            out_specs=(vmem,) * 3,
            scratch_shapes=[
                pltpu.VMEM((draft_rows, vocab), f32),
                pltpu.VMEM((draft_rows, 128), f32),
                pltpu.VMEM((draft_rows, 128), f32),
                pltpu.VMEM((draft_rows, 128), f32),
                pltpu.VMEM((n, 2, 8, 128), f32),
                pltpu.VMEM((8, 128), f32),
                pltpu.VMEM((n, 8, 128), f32),
                pltpu.SemaphoreType.DMA((draft_rows // 8,)),
                pltpu.SemaphoreType.DMA((n,)),
                pltpu.SemaphoreType.DMA((n,)),
                pltpu.SemaphoreType.DMA((n,)),
                pltpu.SemaphoreType.DMA((n,)),
            ],
            compiler_params=pltpu.CompilerParams(
                collective_id=0, has_side_effects=True, vmem_limit_bytes=16 * 2**20),
            name='exchange',
        )(*[pltpu.with_memory_space_constraint(a, pltpu.VMEM) for a in made],
          pltpu.with_memory_space_constraint(q, pltpu.HBM))
        slots = 8
        residual, accept, norm_sum, bonus = pl.pallas_call(
            _scale_kernel,
            out_shape=(jax.ShapeDtypeStruct((draft_rows, vocab), f32),
                       jax.ShapeDtypeStruct((draft, seqs), f32),
                       jax.ShapeDtypeStruct((draft, seqs), f32),
                       jax.ShapeDtypeStruct((1, seqs), f32)),
            in_specs=[vmem, vmem, vmem],
            out_specs=(hbm,) * 4,
            scratch_shapes=[pltpu.VMEM((slots, 8, vocab), f32), pltpu.VMEM((3, 4, seqs), f32),
                            pltpu.SemaphoreType.DMA((slots,)), pltpu.SemaphoreType.DMA((3,))],
            compiler_params=pltpu.CompilerParams(vmem_limit_bytes=8 * 2**20),
            name='scale',
        )(*[pltpu.with_memory_space_constraint(a, pltpu.VMEM) for a in (z, norm, stat)])
        residual = residual.reshape(draft, seqs, vocab).transpose(1, 0, 2)
        return accept.T, norm_sum.T, residual, bonus[0]

    return jax.shard_map(
        local_step,
        mesh=mesh,
        in_specs=(P('dp', None, None), P(), P(None, 'tp'), P('dp', None, 'tp'), P('dp', None), P('dp')),
        out_specs=(P('dp', None), P('dp', None), P('dp', None, 'tp'), P('dp')),
        check_vma=False,
    )
```

```python
import functools

import jax
import jax.numpy as jnp
from jax import lax
from jax.experimental import pallas as pl
from jax.experimental.pallas import tpu as pltpu
from jax.sharding import PartitionSpec as P

LOG2E = 1.4426950408889634
LN2 = 0.6931471805599453
MESH = pl.DeviceIdType.MESH
TILE = 512
DEPTH = 8
EARLY = 2
BLOCK = 32
LOW = -3.0e38


def _pack(packed, g, col):
    lane = lax.broadcasted_iota(jnp.int32, (8, 128), 1)
    return jnp.where((lane == g) | (lane == g + 32), col, packed)


def _stream_kernel(h_ref, gain_ref, temp_ref, tok_ref, w_ref,
                   z_ref, ml_ref, k_ref, mk_ref, kp_ref, hit_ref,
                   hbuf, gbuf, tbuf, dbuf, hp_ref, x_ref, wbuf, wtail, m_ref, l_ref,
                   wsem, tsem, isem):
    me = lax.axis_index('tp')
    vocab = w_ref.shape[0]
    width = w_ref.shape[1]
    seqs = h_ref.shape[0]
    rows = seqs * 4
    per = seqs // 8
    draft_rows = rows - seqs
    groups = draft_rows // 8
    all_groups = rows // 8
    tiles = vocab // TILE
    tail = vocab - tiles * TILE
    tail_at = tiles * TILE
    chunks = width // 256
    lane = lax.broadcasted_iota(jnp.int32, (8, 128), 1)
    sub = lax.broadcasted_iota(jnp.int32, (8, 128), 0)

    def w_copy(tile):
        slot = lax.rem(tile, DEPTH)
        return pltpu.make_async_copy(
            w_ref.at[pl.ds(pl.multiple_of(tile * TILE, TILE), TILE), :], wbuf.at[slot], wsem.at[slot])

    first_copies = [pltpu.make_async_copy(a, b, isem.at[i]) for i, (a, b) in enumerate(
        ((h_ref, hbuf), (temp_ref, tbuf), (gain_ref, gbuf), (tok_ref, dbuf)))]
    for copy in first_copies:
        copy.start()
    tail_copy = pltpu.make_async_copy(w_ref.at[pl.ds(tail_at, tail), :], wtail.at[pl.ds(0, tail), :], tsem)
    tail_copy.start()
    for i in range(EARLY):
        w_copy(i).start()

    m_ref[...] = jnp.full_like(m_ref, LOW)
    l_ref[...] = jnp.zeros_like(l_ref)
    wtail[tail:, :] = jnp.zeros((wtail.shape[0] - tail, width), wtail.dtype)

    for copy in first_copies[1:]:
        copy.wait()

    def column(row, g):
        picked = jnp.where(lane[:, :seqs] == g * 8 + sub[:, :seqs], jnp.broadcast_to(row, (8, seqs)), 0.0)
        return jnp.sum(picked, axis=1, keepdims=True)

    kp = jnp.zeros((8, 128), jnp.float32)
    for g in range(per):
        k = jnp.broadcast_to(LOG2E / column(tbuf[...], g), (8, 128))
        k_ref[g * 8:g * 8 + 8, :] = k
        kp = jnp.where(lax.rem(lane, per) == g, k, kp)
    for j in range(3):
        row = (dbuf[j:j + 1, :] - me * vocab).astype(jnp.float32)
        for g in range(per):
            at = slice(j * seqs + g * 8, j * seqs + g * 8 + 8)
            hit_ref[at, :] = jnp.broadcast_to(column(row, g), (8, 128)).astype(jnp.int32)
    kp_ref[...] = kp
    first_copies[0].wait()
    for i in range(EARLY, DEPTH - 1):
        w_copy(i).start()

    def run(*accs):
        def acc(q, p, b):
            return accs[(q * 2 + p) * 4 + b]

        def accumulate(q, p, c, staged=None):
            staged = c % 2 if staged is None else staged
            for b in range(4):
                pltpu.matmul_acc_lhs(
                    acc(q, p, b), x_ref[b * seqs:(b + 1) * seqs, c * 256:(c + 1) * 256],
                    load_staged_rhs=staged if b == 0 else None)

        def push(tile, q, c):
            slot = lax.rem(tile, DEPTH)
            pltpu.matmul_push_rhs(
                wbuf[slot, q * 256:(q + 1) * 256, c * 256:(c + 1) * 256],
                staging_register=c % 2, mxu_index=q, transpose=True)

        cols = lax.broadcasted_iota(jnp.int32, (seqs, 128), 1)

        def update(b, parts):
            at = slice(b * seqs, (b + 1) * seqs)
            k = k_ref[...]
            old = m_ref[at, :]
            new = old
            for v in parts:
                new = jnp.maximum(new, v)
            total = l_ref[at, :] * jnp.exp2((old - new) * k)
            for v in parts:
                total = total + jnp.exp2((v - new) * k)
            m_ref[at, :] = new
            l_ref[at, :] = total

        def drain(tile, p, b):
            parts = []
            for q in range(2):
                v = pltpu.matmul_pop(acc(q, p, b))
                if b < 3:
                    at = pl.ds(pl.multiple_of(tile * TILE + q * 256, 256), 256)
                    z_ref[b * seqs:(b + 1) * seqs, at] = v
                parts += [v[:, :128], v[:, 128:]]
            update(b, parts)

        def drain_tail(p, b):
            v = pltpu.matmul_pop(acc(0, p, b)) + pltpu.matmul_pop(acc(1, p, b))
            if b < 3:
                z_ref[b * seqs:(b + 1) * seqs, tail_at:tail_at + tail] = v[:, :tail]
            update(b, [jnp.where(cols < tail, v[:, :128], LOW)])

        def step(tile, p, last=False, first=False, refill=None):
            if not last:
                w_copy(tile + 1).wait()
            if refill is not None:
                refill()
            for c in range(chunks):
                for q in range(2):
                    accumulate(q, p, c)
                for q in range(2):
                    if c + 1 < chunks:
                        push(tile, q, c + 1)
                    elif not last:
                        push(tile + 1, q, 0)
                if 1 <= c <= 4:
                    if first:
                        drain_tail(1 - p, c - 1)
                    else:
                        drain(tile - 1, 1 - p, c - 1)

        c_of = lax.broadcasted_iota(jnp.int32, (seqs, 256), 1)
        r_of = lax.broadcasted_iota(jnp.int32, (seqs, 256), 0)
        def reorder(c):
            flat = hbuf[:, :, c * 256:(c + 1) * 256].reshape(rows, 256)
            pltpu.matmul_push_rhs(flat, staging_register=(c // 2) % 2, mxu_index=c % 2)
            for b in range(4):
                pick = jnp.where(c_of == r_of * 4 + b, 1.0, 0.0).astype(jnp.bfloat16)
                pltpu.matmul_acc_lhs(acc(c % 2, (c // 2) % 2, b), pick,
                                     load_staged_rhs=(c // 2) % 2 if b == 0 else None)

        def reordered(c):
            for b in range(4):
                hp_ref[b * seqs:(b + 1) * seqs, c * 256:(c + 1) * 256] = pltpu.matmul_pop(acc(c % 2, (c // 2) % 2, b))

        for c in range(chunks):
            if c >= 4:
                reordered(c - 4)
            reorder(c)
        for c in range(max(0, chunks - 4), chunks):
            reordered(c)
        gain = gbuf[...]
        for g in range(all_groups // 2):
            at = slice(g * 16, g * 16 + 16)
            h = hp_ref[at, :]
            inv_rms = lax.rsqrt(jnp.sum(h * h, axis=1, keepdims=True) * (1.0 / width) + 1e-5)
            for c in range(width // 128):
                cs = slice(c * 128, c * 128 + 128)
                x_ref[at, cs] = (h[:, cs] * inv_rms * gain[c:c + 1, :]).astype(jnp.bfloat16)

        tail_copy.wait()
        half = chunks // 2
        for i in range(half):
            for q in range(2):
                c = q * half + i
                pltpu.matmul_push_rhs(wtail[:, c * 256:(c + 1) * 256], staging_register=i % 2, mxu_index=q, transpose=True)
                accumulate(q, 1, c, i % 2)
        w_copy(0).wait()
        for q in range(2):
            push(0, q, 0)
        step(0, 0, first=True, refill=lambda: w_copy(DEPTH - 1).start())

        def refill_at(tile):
            @pl.when(tile + DEPTH - 1 < tiles)
            def _():
                w_copy(tile + DEPTH - 1).start()

        @pl.loop(0, (tiles - 3) // 2)
        def _(t):
            tile = 1 + 2 * t
            step(tile, 1, refill=lambda: refill_at(tile))
            step(tile + 1, 0, refill=lambda: refill_at(tile + 1))

        step(tiles - 2, 1)
        step(tiles - 1, 0, last=True)
        for b in range(4):
            drain(tiles - 1, 0, b)

    pl.run_scoped(run, *[pltpu.ACC(q)((seqs, 256), jnp.float32) for q in range(2) for _ in range(8)])

    packed_m = jnp.zeros((8, 128), jnp.float32)
    packed_l = jnp.zeros((8, 128), jnp.float32)
    for g in range(all_groups):
        at = slice(g * 8, g * 8 + 8)
        m = m_ref[at, :]
        top = jnp.max(m, axis=1, keepdims=True)
        k = k_ref[g % per * 8:g % per * 8 + 8, :]
        total = jnp.sum(l_ref[at, :] * jnp.exp2((m - top) * k), axis=1, keepdims=True)
        packed_m = _pack(packed_m, g, top)
        if g < groups:
            mk_ref[at, :] = top * k
        packed_l = _pack(packed_l, g, total)
    ml_ref[0] = packed_m
    ml_ref[1] = packed_l


def _exchange_kernel(n, z_ref, ml_ref, k_ref, mk_ref, kp_ref, hit_ref, q_ref, e_ref, stat_ref,
                     y_ref, scale_ref, part_q, part_z, recv1, send2, recv2, qsem, ssem1, rsem1, ssem2, rsem2):
    me = lax.axis_index('tp')
    dp = lax.axis_index('dp')
    draft_rows, vocab = q_ref.shape
    groups = draft_rows // 8
    per = k_ref.shape[0] // 8
    full = vocab // 128
    rest = vocab - full * 128
    edge = slice(full * 128, vocab)
    lane = lax.broadcasted_iota(jnp.int32, (8, 128), 1)

    def q_copy(g):
        at = pl.ds(pl.multiple_of(g * 8, 8), 8)
        return pltpu.make_async_copy(q_ref.at[at, :], e_ref.at[at, :], qsem.at[g])

    barrier = pltpu.get_barrier_semaphore()
    for d in range(1, n):
        pl.semaphore_signal(barrier, inc=1, device_id=(dp, lax.rem(me + d, n)), device_id_type=MESH)
    for g in range(groups):
        q_copy(g).start()
    recv1[me] = ml_ref[...]
    pl.semaphore_wait(barrier, n - 1)

    def share(src, dst, ssem, rsem):
        copies = []
        for d in range(1, n):
            copy = pltpu.make_async_remote_copy(
                src_ref=src, dst_ref=dst.at[me], send_sem=ssem.at[d], recv_sem=rsem.at[me],
                device_id=(dp, lax.rem(me + d, n)), device_id_type=MESH)
            copy.start()
            copies.append(copy)
        return copies

    def collect(src, dst, ssem, rsem):
        for d in range(1, n):
            peer = lax.rem(me + d, n)
            pltpu.make_async_remote_copy(
                src_ref=src, dst_ref=dst.at[peer], send_sem=ssem.at[d], recv_sem=rsem.at[peer],
                device_id=(dp, peer), device_id_type=MESH).wait_recv()

    copies1 = share(ml_ref, recv1, ssem1, rsem1)

    @pl.loop(0, groups)
    def _(g):
        q_copy(g).wait()
        at = pl.ds(pl.multiple_of(g * 8, 8), 8)
        hit = hit_ref[at, :]
        k = k_ref[pl.ds(pl.multiple_of(lax.rem(g, per) * 8, 8), 8), :]
        mk = mk_ref[at, :]
        got_q = [jnp.zeros((8, 128), jnp.float32) for _ in range(2)]
        got_z = [jnp.zeros((8, 128), jnp.float32) for _ in range(2)]
        for c in range(full):
            cols = slice(c * 128, c * 128 + 128)
            here = hit - c * 128 == lane
            z = z_ref[at, cols]
            y_ref[at, cols] = jnp.exp2(z * k - mk)
            got_q[c % 2] = jnp.where(here, e_ref[at, cols], got_q[c % 2])
            got_z[c % 2] = jnp.where(here, z, got_z[c % 2])
        y_ref[at, edge] = jnp.exp2(z_ref[at, edge] * k[:, :rest] - mk[:, :rest])
        here = hit[:, :rest] - full * 128 == lane[:, :rest]
        part_q[at, :] = got_q[0] + got_q[1]
        part_z[at, :] = got_z[0] + got_z[1]
        part_q[at, :rest] = part_q[at, :rest] + jnp.where(here, e_ref[at, edge], 0.0)
        part_z[at, :rest] = part_z[at, :rest] + jnp.where(here, z_ref[at, edge], 0.0)

    tok_q = jnp.zeros((8, 128), jnp.float32)
    tok_z = jnp.zeros((8, 128), jnp.float32)
    for g in range(groups):
        at = slice(g * 8, g * 8 + 8)
        tok_q = _pack(tok_q, g, jnp.sum(part_q[at, :], axis=1, keepdims=True))
        tok_z = _pack(tok_z, g, jnp.sum(part_z[at, :], axis=1, keepdims=True))

    collect(ml_ref, recv1, ssem1, rsem1)
    kp = kp_ref[...]
    top = recv1[0, 0]
    for i in range(1, n):
        top = jnp.maximum(top, recv1[i, 0])
    total = jnp.zeros((8, 128), jnp.float32)
    for i in range(n):
        total = total + recv1[i, 1] * jnp.exp2((recv1[i, 0] - top) * kp)
    lse = top * kp + jnp.log(total) * LOG2E
    stat_ref[1] = lse * LN2
    for g in range(groups):
        col = jnp.sum(jnp.where(lane == g, lse, 0.0), axis=1, keepdims=True)
        scale_ref[g * 8:g * 8 + 8, :] = jnp.exp2(mk_ref[g * 8:g * 8 + 8, :] - col)

    @pl.loop(0, draft_rows // BLOCK)
    def _(i):
        at = pl.ds(pl.multiple_of(i * BLOCK, BLOCK), BLOCK)
        base = scale_ref[at, :]
        sums = [jnp.zeros((BLOCK, 128), jnp.float32) for _ in range(2)]
        for c in range(full):
            cols = slice(c * 128, c * 128 + 128)
            e = jnp.maximum(y_ref[at, cols] * base - e_ref[at, cols], 0.0)
            e_ref[at, cols] = e
            sums[c % 2] = sums[c % 2] + e
        e = jnp.maximum(y_ref[at, edge] * base[:, :rest] - e_ref[at, edge], 0.0)
        e_ref[at, edge] = e
        part_q[at, :] = sums[0] + sums[1]
        part_q[at, :rest] = part_q[at, :rest] + e

    packed = jnp.zeros((8, 128), jnp.float32)
    for g in range(groups):
        packed = _pack(packed, g, jnp.sum(part_q[g * 8:g * 8 + 8, :], axis=1, keepdims=True))
    below = jnp.where(tok_q > 0, tok_q, 1.0)
    accept = jnp.where(tok_q > 0, jnp.minimum(1.0, jnp.exp2(tok_z * kp - lse) / below), 0.0)
    packed = jnp.where((lane >= 32) & (lane < 64), accept, packed)
    send2[...] = packed
    recv2[me] = packed
    copies2 = share(send2, recv2, ssem2, rsem2)
    collect(send2, recv2, ssem2, rsem2)
    total = recv2[0]
    for i in range(1, n):
        total = total + recv2[i]
    stat_ref[0] = total
    for copy in copies1 + copies2:
        copy.wait_send()


def _scale_kernel(e_ref, stat_ref, o_ref, accept_ref, sum_ref, bonus_ref, stage, small, sem, ssem):
    rows, vocab = o_ref.shape
    full = vocab // 128
    slots = stage.shape[0]
    seqs = bonus_ref.shape[1]
    per = seqs // 8
    count = rows // 8

    def out_copy(g, slot):
        at = pl.ds(pl.multiple_of(g * 8, 8), 8)
        return pltpu.make_async_copy(stage.at[slot], o_ref.at[at, :], sem.at[slot])

    lane = lax.broadcasted_iota(jnp.int32, (8, 128), 1)
    sub = lax.broadcasted_iota(jnp.int32, (8, 128), 0)
    inverse = 1.0 / stat_ref[0]

    def scale(g):
        slot = lax.rem(g, slots)
        at = pl.ds(pl.multiple_of(g * 8, 8), 8)
        inv = jnp.broadcast_to(jnp.sum(jnp.where(lane == g, inverse, 0.0), axis=1, keepdims=True), (8, 128))
        for c in range(full):
            cols = slice(c * 128, c * 128 + 128)
            stage[slot, :, cols] = e_ref[at, cols] * inv
        cols = slice(full * 128, vocab)
        stage[slot, :, cols] = e_ref[at, cols] * inv[:, :vocab - full * 128]
        out_copy(g, slot).start()

    @pl.loop(0, slots)
    def _(g):
        scale(g)

    def spread(packed, first):
        row = jnp.zeros((8, 128), jnp.float32)
        for g in range(per):
            col = jnp.sum(jnp.where(lane == first + g, packed, 0.0), axis=1, keepdims=True)
            row = jnp.where(lane == g * 8 + sub, col, row)
        return jnp.sum(row, axis=0, keepdims=True)[:, :seqs]

    draft = accept_ref.shape[0]
    for j in range(draft):
        small[0, j:j + 1, :] = spread(stat_ref[0], 32 + j * per)
        small[1, j:j + 1, :] = spread(stat_ref[0], j * per)
    small[2, 0:1, :] = spread(stat_ref[1], count)
    smalls = [pltpu.make_async_copy(small.at[0, pl.ds(0, draft), :], accept_ref, ssem.at[0]),
              pltpu.make_async_copy(small.at[1, pl.ds(0, draft), :], sum_ref, ssem.at[1]),
              pltpu.make_async_copy(small.at[2, pl.ds(0, 1), :], bonus_ref, ssem.at[2])]

    @pl.loop(slots, count)
    def _(g):
        out_copy(g - slots, lax.rem(g, slots)).wait()
        scale(g)

        @pl.when(g == slots)
        def _():
            for copy in smalls:
                copy.start()

    for copy in smalls:
        copy.wait()
    for i in range(slots):
        out_copy(count - slots + i, lax.rem(count - slots + i, slots)).wait()


def solution(mesh):
    n = mesh.shape['tp']

    def local_step(hidden, norm_gain, w_head, draft_probs, draft_tokens, temperature):
        seqs, positions, width = hidden.shape
        vocab = w_head.shape[1]
        rows = seqs * positions
        draft = positions - 1
        draft_rows = seqs * draft
        q = draft_probs.transpose(1, 0, 2).reshape(draft_rows, vocab)
        vmem = pl.BlockSpec(memory_space=pltpu.VMEM)
        hbm = pl.BlockSpec(memory_space=pltpu.HBM)
        f32 = jnp.float32
        made = pl.pallas_call(
            _stream_kernel,
            out_shape=(pltpu.VMEM((draft_rows, vocab), f32),
                       pltpu.VMEM((2, 8, 128), f32),
                       pltpu.VMEM((seqs, 128), f32),
                       pltpu.VMEM((draft_rows, 128), f32),
                       pltpu.VMEM((8, 128), f32),
                       pltpu.VMEM((draft_rows, 128), jnp.int32)),
            in_specs=[hbm] * 5,
            out_specs=(vmem,) * 6,
            scratch_shapes=[
                pltpu.VMEM((seqs, positions, width), jnp.bfloat16),
                pltpu.VMEM((width // 128, 128), f32),
                pltpu.VMEM((1, seqs), f32),
                pltpu.VMEM((draft, seqs), jnp.int32),
                pltpu.VMEM((rows, width), f32),
                pltpu.VMEM((rows, width), jnp.bfloat16),
                pltpu.VMEM((DEPTH, TILE, width), jnp.bfloat16),
                pltpu.VMEM((256, width), jnp.bfloat16),
                pltpu.VMEM((rows, 128), f32),
                pltpu.VMEM((rows, 128), f32),
                pltpu.SemaphoreType.DMA((DEPTH,)),
                pltpu.SemaphoreType.DMA,
                pltpu.SemaphoreType.DMA((4,)),
            ],
            compiler_params=pltpu.CompilerParams(vmem_limit_bytes=28 * 2**20),
            name='stream',
        )(*[pltpu.with_memory_space_constraint(a, pltpu.HBM) for a in (
            hidden, norm_gain.reshape(width // 128, 128), temperature[None], draft_tokens.T, w_head.T)])
        z, stat = pl.pallas_call(
            functools.partial(_exchange_kernel, n),
            out_shape=(pltpu.VMEM((draft_rows, vocab), f32),
                       pltpu.VMEM((2, 8, 128), f32)),
            in_specs=[vmem] * 6 + [hbm],
            out_specs=(vmem,) * 2,
            scratch_shapes=[
                pltpu.VMEM((draft_rows, vocab), f32),
                pltpu.VMEM((draft_rows, 128), f32),
                pltpu.VMEM((draft_rows, 128), f32),
                pltpu.VMEM((draft_rows, 128), f32),
                pltpu.VMEM((n, 2, 8, 128), f32),
                pltpu.VMEM((8, 128), f32),
                pltpu.VMEM((n, 8, 128), f32),
                pltpu.SemaphoreType.DMA((draft_rows // 8,)),
                pltpu.SemaphoreType.DMA((n,)),
                pltpu.SemaphoreType.DMA((n,)),
                pltpu.SemaphoreType.DMA((n,)),
                pltpu.SemaphoreType.DMA((n,)),
            ],
            compiler_params=pltpu.CompilerParams(
                collective_id=0, has_side_effects=True, vmem_limit_bytes=16 * 2**20),
            name='exchange',
        )(*[pltpu.with_memory_space_constraint(a, pltpu.VMEM) for a in made],
          pltpu.with_memory_space_constraint(q, pltpu.HBM))
        slots = 8
        residual, accept, norm_sum, bonus = pl.pallas_call(
            _scale_kernel,
            out_shape=(jax.ShapeDtypeStruct((draft_rows, vocab), f32),
                       jax.ShapeDtypeStruct((draft, seqs), f32),
                       jax.ShapeDtypeStruct((draft, seqs), f32),
                       jax.ShapeDtypeStruct((1, seqs), f32)),
            in_specs=[vmem, vmem],
            out_specs=(hbm,) * 4,
            scratch_shapes=[pltpu.VMEM((slots, 8, vocab), f32), pltpu.VMEM((3, 4, seqs), f32),
                            pltpu.SemaphoreType.DMA((slots,)), pltpu.SemaphoreType.DMA((3,))],
            compiler_params=pltpu.CompilerParams(vmem_limit_bytes=8 * 2**20),
            name='scale',
        )(*[pltpu.with_memory_space_constraint(a, pltpu.VMEM) for a in (z, stat)])
        residual = residual.reshape(draft, seqs, vocab).transpose(1, 0, 2)
        return accept.T, norm_sum.T, residual, bonus[0]

    return jax.shard_map(
        local_step,
        mesh=mesh,
        in_specs=(P('dp', None, None), P(), P(None, 'tp'), P('dp', None, 'tp'), P('dp', None), P('dp')),
        out_specs=(P('dp', None), P('dp', None), P('dp', None, 'tp'), P('dp')),
        check_vma=False,
    )
```
